128 devices in a mesh: gx: 16 (over x, y), gy: 8 (over z, core).
Axes of the slice: x: 4, y: 4, z: 4, core: 2. Of those that a mesh axis runs over, the one named last changes fastest.
Arguments:
- thermal_state: bfloat16 [98304, 4096], P(('gx', 'gy')), may hold values from 0.59765625 to 1.3984375
- opacity_field: bfloat16 [98304, 4096], P(('gx', 'gy')), may hold values from 0.15 to 4.5
- glowing_depth: int32 [98304], P(('gx', 'gy')), may hold values from 1 to 16
- position_to_tile: int32 [98304], P(('gx', 'gy')), may hold values from 0 to 98303, as said below
- tile_to_position: int32 [98304], P(('gx', 'gy')), may hold values from 0 to 98303, as said below
Outputs:
- heating: float32 [98304, 4096], P(('gx', 'gy'))
The draws below stay inside these ranges and needn't reach their ends.
Inputs may be any that keep to these rules, and one draw needn't show every extreme that they name: `position_to_tile`: A permutation. Box q belongs to column q // 768. The 768 slots s with the same s // 768 hold boxes of exactly half of the 128 columns, exactly 12 boxes of each of those. tile_to_position[position_to_tile[s]] = s for every slot s.
All inputs are finite; a program needn't handle non-finite values.
Results may differ from the reference program's by a relative error of at most 0.0003.
Values sent between devices are 32-bit elements; how exact they have to be, the bound alone decides.
A program may use at most 128 MiB of HBM per device.

```python
import math
import jax
import jax.numpy as jnp
import numpy as np
from jax import lax

CB = 4
RF = 4
SWEEPS = 4
CX = 16
CY = 24
CZ = 128
EDGE_RESOLUTION = 16
NBX = 4
NBY = 6
NBZ = 32
COLX = 16
COLY = 8
STACK_DEPTH = 768
DOMAIN_TILES = 98304
CAP = 12
NXC = 256
NYC = 192


def shuffled_rows(key, row_count, row_length):

    def one_row(row_key):
        return jax.random.permutation(row_key, row_length)
    return jax.vmap(one_row)(jax.random.split(key, row_count))


def assignment(key):
    owners = DOMAIN_TILES // STACK_DEPTH
    groups = owners // 2
    key_start, key_shift, key_local, key_order = jax.random.split(jax.random.fold_in(key, 11), 4)
    start_of = jax.random.permutation(key_start, owners)
    shift_of = jax.random.permutation(key_shift, owners)[:groups]
    local_rank = shuffled_rows(key_local, owners, STACK_DEPTH)
    group_of = local_rank // CAP
    within_group = local_rank % CAP
    flame_dev = (start_of[:, None] + shift_of[group_of]) % owners
    slot_order = shuffled_rows(key_order, owners, STACK_DEPTH)
    slot_local = slot_order[flame_dev, group_of * CAP + within_group]
    slot_of_box = (flame_dev * STACK_DEPTH + slot_local).reshape(-1).astype(jnp.int32)
    box_of_slot = jnp.zeros((DOMAIN_TILES,), jnp.int32).at[slot_of_box].set(jnp.arange(DOMAIN_TILES, dtype=jnp.int32))
    return (box_of_slot, slot_of_box)


def draw_position_to_tile(key, part):
    return assignment(key)[0]


def draw_tile_to_position(key, part):
    return assignment(key)[1]


def draw_opacity_field(key, part):
    box_of_slot = assignment(key)[0]
    boxes_x = CX // CB
    boxes_y = CY // CB
    boxes_z = CZ // CB
    column = box_of_slot // STACK_DEPTH
    within_column = box_of_slot % STACK_DEPTH
    place_x = column // COLY * boxes_x + within_column // (boxes_y * boxes_z)
    place_y = column % COLY * boxes_y + within_column // boxes_z % boxes_y
    trend = place_x.astype(jnp.float32) / (COLX * boxes_x) + place_y.astype(jnp.float32) / (COLY * boxes_y)
    fine_index = jnp.arange(EDGE_RESOLUTION ** 3, dtype=jnp.int32)
    cell_x = fine_index // (EDGE_RESOLUTION * EDGE_RESOLUTION) // RF
    cell_y = fine_index // EDGE_RESOLUTION % EDGE_RESOLUTION // RF
    cell_z = fine_index % EDGE_RESOLUTION // RF
    cell_index = (cell_x * CB + cell_y) * CB + cell_z
    cell_key = jax.random.fold_in(key, 31)
    cell_factor = jnp.exp(jax.random.uniform(cell_key, (DOMAIN_TILES, CB ** 3), jnp.float32, math.log(0.5), math.log(2.0)))
    rough = jnp.take(cell_factor, cell_index, axis=1)
    noise_key = jax.random.fold_in(key, 23)
    factor = jnp.exp(jax.random.uniform(noise_key, (DOMAIN_TILES, EDGE_RESOLUTION ** 3), jnp.float32, math.log(0.8), math.log(1.25)))
    scale = 0.4 * jnp.power(3.0, 0.5 * trend)
    return (scale[:, None] * rough * factor).astype(jnp.bfloat16)


def place_ends(array, own_key, low, largest):
    longest = array.shape.index(max(array.shape))
    spots = []
    for shift in (0, 1):
        where = [jax.random.randint(jax.random.fold_in(own_key, axis), (), 0, length) for axis, length in enumerate(array.shape)]
        where[longest] = (where[longest] + shift) % array.shape[longest]
        spots.append(tuple(where))
    return array.at[spots[0]].set(low).at[spots[1]].set(largest)


def block_scale(rng, extent, shards, low, high):
    loudness, own = 1.0, jax.random.fold_in(rng, 6)
    for dim, parts in shards:
        heights = jnp.exp(jax.random.uniform(jax.random.fold_in(own, dim), (parts,), jnp.float32, low / len(shards), high / len(shards)))
        loudness = loudness * jnp.repeat(heights, extent[dim] // parts).reshape([-1 if axis == dim else 1 for axis in range(len(extent))])
    return loudness


def setup_inputs(seed: int = 0) -> dict:
    key_list = jax.random.split(jax.random.key(seed), 6)
    return {
        "thermal_state": jnp.clip(jnp.exp(math.log(1.3984375) - 0.8500951 * jax.random.uniform(key_list[0], (DOMAIN_TILES, EDGE_RESOLUTION**3), jnp.float32) ** block_scale(key_list[0], (DOMAIN_TILES, EDGE_RESOLUTION**3), ((0, 128),), -0.2, 0.2)), 0.59765625, 1.3984375).astype(jnp.bfloat16),
        "opacity_field": draw_opacity_field(jax.random.fold_in(key_list[5], 71), 0),
        "glowing_depth": place_ends(jax.random.randint(key_list[2], (DOMAIN_TILES,), 1, EDGE_RESOLUTION + 1), jax.random.fold_in(key_list[2], 1), 1, EDGE_RESOLUTION).astype(jnp.int32),
        "position_to_tile": draw_position_to_tile(jax.random.fold_in(key_list[5], 71), 0),
        "tile_to_position": draw_tile_to_position(jax.random.fold_in(key_list[5], 71), 0),
    }


EXACT_DOT = lax.Precision.HIGHEST


def restrict_table():
    fine_index = np.arange(EDGE_RESOLUTION ** 3)
    coarse_x = fine_index // (EDGE_RESOLUTION * EDGE_RESOLUTION) // RF
    coarse_y = fine_index // EDGE_RESOLUTION % EDGE_RESOLUTION // RF
    coarse_z = fine_index % EDGE_RESOLUTION // RF
    coarse_index = (coarse_x * CB + coarse_y) * CB + coarse_z
    averaging = (coarse_index[:, None] == np.arange(CB ** 3)[None, :]) / float(RF ** 3)
    return jnp.asarray(averaging, jnp.float32)


def spread_table():
    border = CB + 2
    line_weights = np.zeros((EDGE_RESOLUTION, border))
    for offset in range(EDGE_RESOLUTION):
        position = (offset + 0.5) / RF + 0.5
        lower_cell = int(np.floor(position))
        upper_share = position - lower_cell
        line_weights[offset, lower_cell] += 1.0 - upper_share
        line_weights[offset, lower_cell + 1] += upper_share
    tensor_weights = np.kron(np.kron(line_weights, line_weights), line_weights)
    return jnp.asarray(tensor_weights.T, jnp.float32)


def cut_windows(coarse_grid, span_x, span_y, span_z):
    border = CB + 2
    along_x = jnp.stack([coarse_grid[offset:offset + span_x:CB] for offset in range(border)], axis=1)
    along_y = jnp.stack([along_x[:, :, offset:offset + span_y:CB] for offset in range(border)], axis=3)
    along_z = jnp.stack([along_y[..., offset:offset + span_z:CB] for offset in range(border)], axis=5)
    return along_z.transpose(0, 2, 4, 1, 3, 5).reshape(-1, border ** 3)


def face_weight(first, second):
    return 2.0 / (3.0 * (first + second))


def emitting_terms(temper, absorb, layers):
    layer_index = jnp.arange(EDGE_RESOLUTION ** 3, dtype=jnp.int32) % EDGE_RESOLUTION
    emitting = (layer_index[None, :] < layers[:, None]).astype(jnp.float32)
    absorb_f = absorb.astype(jnp.float32)
    thermal_forcing = temper.astype(jnp.float32)
    square = thermal_forcing * thermal_forcing
    fourth = square * square * emitting
    return absorb_f, fourth


def reference(thermal_state, opacity_field, glowing_depth, position_to_tile, tile_to_position):
    voxel_number = EDGE_RESOLUTION ** 3
    payload = 2 * CB ** 3
    averaging = restrict_table()
    tile_sequence = DOMAIN_TILES // STACK_DEPTH

    def restrict_tile(pieces):
        absorb_f, fourth = emitting_terms(pieces[0], pieces[1], pieces[2])
        emission = absorb_f * fourth
        return jnp.concatenate([jnp.dot(emission, averaging, precision=EXACT_DOT),
                                jnp.dot(absorb_f, averaging, precision=EXACT_DOT)], axis=1)

    restricted_glow = lax.map(restrict_tile, (thermal_state.reshape(tile_sequence, STACK_DEPTH, voxel_number),
                                          opacity_field.reshape(tile_sequence, STACK_DEPTH, voxel_number),
                                          glowing_depth.reshape(tile_sequence, STACK_DEPTH))).reshape(DOMAIN_TILES, payload)
    by_box = jnp.zeros((DOMAIN_TILES, payload), jnp.float32).at[position_to_tile].set(restricted_glow)
    coarse_grid = by_box.reshape(COLX, COLY, NBX, NBY, NBZ, 2, CB, CB, CB)
    coarse_grid = coarse_grid.transpose(5, 0, 2, 6, 1, 3, 7, 4, 8).reshape(2, NXC, NYC, CZ)
    source = 4.0 * coarse_grid[0]
    coarse_k = coarse_grid[1]

    padded_k = jnp.pad(coarse_k, 1, mode="edge")
    minus_x = face_weight(coarse_k, padded_k[:-2, 1:-1, 1:-1])
    plus_x = face_weight(coarse_k, padded_k[2:, 1:-1, 1:-1])
    minus_y = face_weight(coarse_k, padded_k[1:-1, :-2, 1:-1])
    plus_y = face_weight(coarse_k, padded_k[1:-1, 2:, 1:-1])
    minus_z = face_weight(coarse_k, padded_k[1:-1, 1:-1, :-2])
    plus_z = face_weight(coarse_k, padded_k[1:-1, 1:-1, 2:])
    diagonal = coarse_k + minus_x + plus_x + minus_y + plus_y + minus_z + plus_z
    inverse = 1.0 / diagonal
    lowest = jnp.min(coarse_k / diagonal)
    cheb_delta = 1.0 - lowest
    cheb_sigma = 1.0 / cheb_delta
    cheb_rho = cheb_delta

    def operator(search):
        padded = jnp.pad(search, 1)
        return diagonal * search - (minus_x * padded[:-2, 1:-1, 1:-1] + plus_x * padded[2:, 1:-1, 1:-1]
                                    + minus_y * padded[1:-1, :-2, 1:-1] + plus_y * padded[1:-1, 2:, 1:-1]
                                    + minus_z * padded[1:-1, 1:-1, :-2] + plus_z * padded[1:-1, 1:-1, 2:])

    solution = jnp.zeros_like(source)
    residual = source
    search = inverse * residual
    for sweep_index in range(SWEEPS):
        applied = operator(search)
        solution = solution + search
        residual = residual - applied
        rho_next = 1.0 / (2.0 * cheb_sigma - cheb_rho)
        search = rho_next * cheb_rho * search + (2.0 * rho_next / cheb_delta) * (inverse * residual)
        cheb_rho = rho_next
    incident = solution + search

    rimmed = jnp.pad(incident, 1, mode="edge")
    border = CB + 2
    windows = cut_windows(rimmed, NXC, NYC, CZ)
    windows = windows.reshape(COLX, NBX, COLY, NBY, NBZ, border ** 3).transpose(0, 2, 1, 3, 4, 5)
    windows = windows.reshape(DOMAIN_TILES, border ** 3)
    by_slot = jnp.zeros((DOMAIN_TILES, border ** 3), jnp.float32).at[tile_to_position].set(windows)
    spreading = spread_table()

    def prolong_block(pieces):
        absorb_f, fourth = emitting_terms(pieces[1], pieces[2], pieces[3])
        fine_field = jnp.dot(pieces[0], spreading, precision=EXACT_DOT)
        return absorb_f * (fine_field - 4.0 * fourth)

    heating = lax.map(prolong_block, (by_slot.reshape(tile_sequence, STACK_DEPTH, border ** 3),
                                      thermal_state.reshape(tile_sequence, STACK_DEPTH, voxel_number),
                                      opacity_field.reshape(tile_sequence, STACK_DEPTH, voxel_number),
                                      glowing_depth.reshape(tile_sequence, STACK_DEPTH)))
    return heating.reshape(DOMAIN_TILES, voxel_number)
```

```python
import functools

import jax
import jax.numpy as jnp
import numpy as np
from jax import lax
from jax.experimental import pallas as pl
from jax.experimental.pallas import tpu as pltpu
from jax.sharding import PartitionSpec as P

MESH = pl.DeviceIdType.MESH
F32 = jnp.float32
BF16 = jnp.bfloat16
BX, BY, BZ = 4, 6, 32
CX, CY = 16, 24
SLOTS = 768
NDEV = 128
CAP = 12
PAD = 16
ROWS = 128
XH, YH = 6, 8
EX, EY = CX + 2 * XH, CY + 2 * YH


def average_table():
    table = np.zeros((4, 2, 2, 8, 16, 4, 2, 4, 4), np.float32)
    for i in range(4):
        for bh in range(2):
            for f in range(2):
                for b in range(8):
                    for c in range(16):
                        weight = 1.0 / 16.0 if f == 0 else 1.0 / 64.0
                        table[i, bh, f, b, c, c // 4, f, i, 2 * bh + b // 4] = weight
    return jnp.asarray(table.reshape(8, 256, 128), BF16)


def select_table():
    table = np.zeros((BY, 6, 128, 128), np.float32)
    for v in range(BY):
        for l in range(6):
            for i in range(3):
                for j in range(6):
                    table[v, l, i * 40 + 7 + 4 * v + j, i * 42 + j * 6 + l] = 1.0
    return jnp.asarray(table.reshape(BY, 768, 128), BF16)


def twice_table():
    table = np.zeros((2, 2, 128, 6, 2, 64), np.float32)
    for i in range(6):
        for jl in range(36):
            table[:, i // 3, (i % 3) * 42 + jl, i, :, jl] = 1.0
    return jnp.asarray(table.reshape(512, 768), BF16)


def line_weights():
    weights = np.zeros((16, 6))
    for a in range(16):
        position = (a + 0.5) / 4 + 0.5
        low = int(np.floor(position))
        weights[a, low] += 1.0 - (position - low)
        weights[a, low + 1] += position - low
    return weights


def plane_table():
    w = line_weights()
    plane = np.zeros((2, 64, 256))
    plane[:, :36] = np.kron(w, w).T
    return jnp.asarray(plane.reshape(128, 256), BF16)


def halves(x):
    high = x.astype(BF16)
    return high, (x - high.astype(F32)).astype(BF16)


def dot(a, b):
    return jnp.dot(a, b, preferred_element_type=F32)


def column(row):
    return jnp.broadcast_to(row, (128, 128)).T


def lanes(shape):
    return lax.broadcasted_iota(jnp.int32, shape, len(shape) - 1)


def place(index):
    return (index // 8, index % 8)


def greet_all():
    barrier = pltpu.get_barrier_semaphore()
    gx, gy = lax.axis_index("gx"), lax.axis_index("gy")
    for p in range(16):
        px = (gx + p) % 16
        for t in range(8):
            if p or t:
                pl.semaphore_signal(
                    barrier, inc=1, device_id=(px, (gy + t) % 8), device_id_type=MESH
                )
    return barrier


def peers():
    gx, gy = lax.axis_index("gx"), lax.axis_index("gy")
    x, y, z, c = gx // 4, gx % 4, gy // 2, gy % 2
    xs = [((x + t) % 4) * 4 for t in range(4)]
    ys = [(y + t) % 4 for t in range(4)]
    zs = [((z + t) % 4) * 2 for t in range(4)]
    cs = [(c + t) % 2 for t in range(2)]
    for p in range(1, NDEV):
        q = p * 45 % NDEV
        yield xs[q // 32] + ys[q // 8 % 4], zs[q // 2 % 4] + cs[q % 2]


def rank_row(owner, key):
    owner_c = [column(owner[:, i * 128 : i * 128 + 128]) for i in range(6)]
    key_c = [column(key[:, i * 128 : i * 128 + 128]) for i in range(6)]
    out = []
    for j in range(6):
        ro, rk = owner[:, j * 128 : j * 128 + 128], key[:, j * 128 : j * 128 + 128]
        total = jnp.zeros((128, 128), F32)
        for i in range(6):
            total += jnp.where((owner_c[i] == ro) & (key_c[i] < rk), 1.0, 0.0)
        out.append(jnp.sum(total, axis=0, keepdims=True))
    return jnp.concatenate(out, axis=1)


def index_kernel(p2t_ref, t2p_ref, target_ref, source_ref):
    box = p2t_ref[...].astype(F32)
    owner = jnp.floor((box + 0.5) * (1.0 / SLOTS))
    slot = lanes((1, SLOTS)).astype(F32)
    target_ref[...] = owner * PAD + rank_row(owner, slot)
    slot = t2p_ref[...].astype(F32)
    home = jnp.floor((slot + 0.5) * (1.0 / SLOTS))
    source_ref[...] = home * PAD + rank_row(home, slot)


def one_hot(row, start, count):
    index = lax.broadcasted_iota(jnp.int32, (count, row.shape[1]), 0) + start
    return jnp.where(index.astype(F32) == row, 1.0, 0.0).astype(BF16)


def restrict_kernel(t_ref, k_ref, depth_ref, target_ref, table_ref, out_ref, held):
    step = pl.program_id(0)
    depth = column(depth_ref[...].astype(F32))
    layer = (lanes((128, 128)) % 16).astype(F32)
    mask = jnp.where(layer < depth, 1.0, 0.0)
    total = jnp.zeros((ROWS, 128), F32)
    for i in range(4):
        for bh in range(2):
            glow = absorb = None
            for a in range(4):
                at = (4 * i + a) * 256 + bh * 128
                t = t_ref[:, at : at + 128].astype(F32)
                k = k_ref[:, at : at + 128].astype(F32)
                square = t * t
                term = k * (square * square)
                glow = term if glow is None else glow + term
                absorb = k if absorb is None else absorb + k
            high, low = halves(jnp.concatenate([glow * mask, absorb], axis=1))
            table = table_ref[2 * i + bh]
            total += dot(high, table) + dot(low, table)
    held[pl.ds(pl.multiple_of(step * ROWS, ROWS), ROWS), :] = total

    @pl.when(step == SLOTS // ROWS - 1)
    def _():
        high, low = halves(held[...])
        target = target_ref[...]

        @pl.loop(0, NDEV // 16)
        def _(chunk):
            hot = one_hot(target, chunk * 256, 256)
            block = (dot(hot, high) + dot(hot, low)).reshape(16, PAD, 128)
            out_ref[pl.ds(chunk * 16, 16)] = block[:, :CAP]


def exchange_kernel(x_ref, o_ref, send_sem, recv_sem, local_sem):
    gx, gy = lax.axis_index("gx"), lax.axis_index("gy")
    me = gx * 8 + gy
    barrier = greet_all()
    local = pltpu.make_async_copy(x_ref.at[me], o_ref.at[me], local_sem)
    local.start()
    pl.semaphore_wait(barrier, NDEV - 1)
    send_all(x_ref, o_ref, send_sem, recv_sem)
    local.wait()
    wait_all(x_ref, o_ref, send_sem, recv_sem)


def send_all(x_ref, o_ref, send_sem, recv_sem):
    me = lax.axis_index("gx") * 8 + lax.axis_index("gy")
    for px, py in peers():
        pltpu.make_async_remote_copy(
            src_ref=x_ref.at[px * 8 + py],
            dst_ref=o_ref.at[me],
            send_sem=send_sem,
            recv_sem=recv_sem,
            device_id=(px, py),
            device_id_type=MESH,
        ).start()


def wait_all(x_ref, o_ref, send_sem, recv_sem):
    others = pl.ds(0, NDEV - 1)
    pltpu.make_async_copy(x_ref.at[others], o_ref.at[others], recv_sem).wait()
    pltpu.make_async_copy(x_ref.at[others], o_ref.at[others], send_sem).wait()


def padded_rows(value):
    n = value.shape[0]
    zeros = jnp.zeros((n, PAD - CAP, 128), F32)
    return jnp.concatenate([value, zeros], axis=1).reshape(n * PAD, 128)


def assemble_kernel(arrived_ref, source_ref, grid_ref):
    source = source_ref[...]

    def chunk(c, total):
        rows = padded_rows(arrived_ref[pl.ds(c * 16, 16)])
        high, low = halves(jnp.concatenate([rows[:128].T, rows[128:].T], axis=1))
        hot = one_hot(source, c * 256, 256)
        return total + dot(high, hot) + dot(low, hot)

    total = lax.fori_loop(0, NDEV // 16, chunk, jnp.zeros((128, SLOTS), F32))
    group = lanes((32, 128)) // 32
    for v in range(BY):
        for u in range(BX):
            out = None
            for l in range(4):
                part = total[l * 32 : l * 32 + 32, v * 128 : v * 128 + 128]
                part = pltpu.roll(part, (l - u) * 32 % 128, 1)
                out = part if out is None else jnp.where(group == l, part, out)
            for f in range(2):
                for i in range(4):
                    at = (f * 4 + i) * 4
                    grid_ref[f, 4 * u + i, 4 * v : 4 * v + 4, :] = out[at : at + 4]


def halo_copies(grid_ref, hx_ref, hy_ref, hc_ref, send_sem, recv_sem):
    gx, gy = lax.axis_index("gx"), lax.axis_index("gy")
    up_x, down_x = (gx + 1) % 16, (gx + 15) % 16
    up_y, down_y = (gy + 1) % 8, (gy + 7) % 8
    last_x, first_x = pl.ds(CX - XH, XH), pl.ds(0, XH)
    last_y, first_y = pl.ds(CY - YH, YH), pl.ds(0, YH)
    every = slice(None)
    plan = [
        (grid_ref.at[:, last_x], hx_ref.at[0], (up_x, gy)),
        (grid_ref.at[:, first_x], hx_ref.at[1], (down_x, gy)),
        (grid_ref.at[:, :, last_y], hy_ref.at[0], (gx, up_y)),
        (grid_ref.at[:, :, first_y], hy_ref.at[1], (gx, down_y)),
        (grid_ref.at[:, last_x, last_y], hc_ref.at[0], (up_x, up_y)),
        (grid_ref.at[:, last_x, first_y], hc_ref.at[1], (up_x, down_y)),
        (grid_ref.at[:, first_x, last_y], hc_ref.at[2], (down_x, up_y)),
        (grid_ref.at[:, first_x, first_y], hc_ref.at[3], (down_x, down_y)),
    ]
    return [
        pltpu.make_async_remote_copy(
            src_ref=src,
            dst_ref=dst,
            send_sem=send_sem.at[n],
            recv_sem=recv_sem.at[n],
            device_id=who,
            device_id_type=MESH,
        )
        for n, (src, dst, who) in enumerate(plan)
    ]


def halo_kernel(grid_ref, hx_ref, hy_ref, hc_ref, send_sem, recv_sem):
    gx, gy = lax.axis_index("gx"), lax.axis_index("gy")
    barrier = pltpu.get_barrier_semaphore()
    for dx in (1, 0, 15):
        for dy in (1, 0, 7):
            if dx or dy:
                who = ((gx + dx) % 16, (gy + dy) % 8)
                pl.semaphore_signal(barrier, inc=1, device_id=who, device_id_type=MESH)
    pl.semaphore_wait(barrier, 8)
    copies = halo_copies(grid_ref, hx_ref, hy_ref, hc_ref, send_sem, recv_sem)
    for copy in copies:
        copy.start()
    for copy in copies:
        copy.wait()


def z_lower(v):
    lane = lanes(v.shape)
    return jnp.where(lane < 32, pltpu.roll(v, 33, 1), pltpu.roll(v, 32, 1))


def z_upper(v):
    lane = lanes(v.shape)
    return jnp.where(lane >= 96, pltpu.roll(v, 95, 1), pltpu.roll(v, 96, 1))


def face(a, b):
    return (2.0 / 3.0) / (a + b)


def solve_kernel(
    grid_ref, hx_ref, hy_ref, hc_ref, a_ref, b_ref, c_ref, low_ref, ext, w, v
):
    gx, gy = lax.axis_index("gx"), lax.axis_index("gy")
    own_x, own_y = pl.ds(XH, CX), pl.ds(YH, CY)
    for f in range(2):
        ext[f, own_x, own_y] = grid_ref[f]
        for side, at in ((0, 0), (1, XH + CX)):
            ext[f, pl.ds(at, XH), own_y] = hx_ref[side, f]
        for side, at in ((0, 0), (1, YH + CY)):
            ext[f, own_x, pl.ds(at, YH)] = hy_ref[side, f]
        for n, (atx, aty) in enumerate(
            ((0, 0), (0, YH + CY), (XH + CX, 0), (XH + CX, YH + CY))
        ):
            ext[f, pl.ds(atx, XH), pl.ds(aty, YH)] = hc_ref[n, f]
    shape = (EY, 128)
    row = lax.broadcasted_iota(jnp.int32, shape, 0)
    lane = lanes(shape)
    y_at = gy * CY + row - YH
    has_ym, has_yp = y_at >= 1, y_at <= 8 * CY - 2
    has_zm, has_zp = lane != 0, lane != 127

    def coefficients(x, low):
        x_at = gx * CX + x - XH
        k = ext[1, x]
        has_xm = jnp.broadcast_to(x_at, shape) >= 1
        has_xp = jnp.broadcast_to(x_at, shape) <= 16 * CX - 2
        near = (
            (has_xm, ext[1, x - 1]),
            (has_xp, ext[1, x + 1]),
            (has_ym, pltpu.roll(k, 1, 0)),
            (has_yp, pltpu.roll(k, EY - 1, 0)),
            (has_zm, z_lower(k)),
            (has_zp, z_upper(k)),
        )
        faces = [face(k, jnp.where(has, other, k)) for has, other in near]
        diagonal = k
        for c in faces:
            diagonal = diagonal + c
        inverse = 1.0 / diagonal
        for n, c in enumerate(faces):
            w[n, x] = jnp.where(near[n][0], c * inverse, 0.0)
        v[0, x] = inverse * ext[0, x]
        own = jnp.broadcast_to((x >= XH) & (x < XH + CX), shape)
        return jnp.minimum(low, jnp.where(own, k * inverse, 1.0))

    low = lax.fori_loop(1, EX - 1, coefficients, jnp.ones(shape, F32))
    low_ref[...] = jnp.broadcast_to(
        jnp.min(jnp.min(low[YH : YH + CY], axis=0, keepdims=True), axis=1, keepdims=True),
        low_ref.shape,
    )

    for n in range(4):

        def apply(x, _, n=n):
            mid = v[n, x]
            v[n + 1, x] = (
                w[0, x] * v[n, x - 1]
                + w[1, x] * v[n, x + 1]
                + w[2, x] * pltpu.roll(mid, 1, 0)
                + w[3, x] * pltpu.roll(mid, EY - 1, 0)
                + w[4, x] * z_lower(mid)
                + w[5, x] * z_upper(mid)
            )
            return 0

        lax.fori_loop(2 + n, EX - 2 - n, apply, 0)
    for x in range(CX + 2):
        at = x + XH - 1
        a_ref[x] = v[0, at]
        b_ref[x] = v[1, at] + v[2, at]
        c_ref[x] = v[3, at] + v[4, at]


def lowest_kernel(low_ref, o_ref, send_sem, recv_sem, local_sem):
    me = lax.axis_index("gx") * 8 + lax.axis_index("gy")
    barrier = greet_all()
    local = pltpu.make_async_copy(low_ref, o_ref.at[me], local_sem)
    local.start()
    pl.semaphore_wait(barrier, NDEV - 1)
    for px, py in peers():
        pltpu.make_async_remote_copy(
            src_ref=low_ref,
            dst_ref=o_ref.at[me],
            send_sem=send_sem,
            recv_sem=recv_sem,
            device_id=(px, py),
            device_id_type=MESH,
        ).start()
    local.wait()
    others = pl.ds(0, NDEV - 1)
    pltpu.make_async_copy(o_ref.at[others], o_ref.at[others], recv_sem).wait()
    pltpu.make_async_copy(o_ref.at[others], o_ref.at[others], send_sem).wait()


def pack_kernel(
    a_ref, b_ref, c_ref, lows_ref, source_ref, table_ref, out_ref, inc, win
):
    gx, gy = lax.axis_index("gx"), lax.axis_index("gy")
    lowest = jnp.min(lows_ref[...], axis=0)
    delta = 1.0 - jnp.broadcast_to(lowest, (EY, 128))
    square = delta * delta
    scale = 1.0 / (16.0 - 20.0 * square + 5.0 * square * square)
    outer = 16.0 * scale
    inner = outer - 20.0 * square * scale
    row = lax.broadcasted_iota(jnp.int32, (EY, 128), 0)
    first_row = (row == YH - 1) & jnp.broadcast_to(gy == 0, (EY, 128))
    last_row = (row == YH + CY) & jnp.broadcast_to(gy == 7, (EY, 128))
    for x in range(CX + 2):
        value = a_ref[x] + inner * b_ref[x] + outer * c_ref[x]
        value = jnp.where(first_row, pltpu.roll(value, EY - 1, 0), value)
        inc[x] = jnp.where(last_row, pltpu.roll(value, 1, 0), value)
    inc[0] = jnp.where(jnp.broadcast_to(gx == 0, (EY, 128)), inc[1], inc[0])
    inc[CX + 1] = jnp.where(
        jnp.broadcast_to(gx == 15, (EY, 128)), inc[CX], inc[CX + 1]
    )
    edge = lax.broadcasted_iota(jnp.int32, (32, 128), 0)
    for h in range(2):
        pieces = [[] for _ in range(6)]
        for u in range(BX):
            stack = [inc[4 * u + 3 * h + i] for i in range(3)]
            stack = jnp.concatenate([*stack, jnp.zeros((8, 128), F32)], axis=0).T
            part = [stack[l * 32 : l * 32 + 32] for l in range(4)]
            pieces[0].append(jnp.where(edge == 0, part[0], pltpu.roll(part[3], 1, 0)))
            for l in range(4):
                pieces[l + 1].append(part[l])
            pieces[5].append(jnp.where(edge == 31, part[3], pltpu.roll(part[0], 31, 0)))
        rows = jnp.concatenate([jnp.concatenate(p, axis=0) for p in pieces], axis=1)
        high, low = halves(rows)
        for v in range(BY):
            table = table_ref[v]
            value = dot(high, table) + dot(low, table)
            top, rest = halves(value)
            win[0, v * 128 : v * 128 + 128, h * 128 : h * 128 + 128] = top
            win[1, v * 128 : v * 128 + 128, h * 128 : h * 128 + 128] = rest
    source = source_ref[...]

    @pl.loop(0, NDEV // 16)
    def _(chunk):
        hot = one_hot(source, chunk * 256, 256)
        block = dot(hot, win[0]) + dot(hot, win[1])
        for h in range(2):
            part = block[:, h * 128 : h * 128 + 128].reshape(16, PAD, 128)
            out_ref[pl.ds(chunk * 16, 16), h] = part[:, :CAP]


def prolong_kernel(
    back_ref, target_ref, t_ref, k_ref, depth_ref, twice_ref, plane_ref, out_ref, held
):
    step = pl.program_id(0)

    @pl.when(step == 0)
    def _():
        for h in range(2):
            high, low = halves(padded_rows(back_ref[:, h]))
            held[:, h * 128 : h * 128 + 128] = high
            held[:, 256 + h * 128 : 256 + h * 128 + 128] = low

    target = column(target_ref[...])
    hot = jnp.concatenate(
        [
            jnp.where((lanes((128, 128)) + c * 128).astype(F32) == target, 1.0, 0.0).astype(BF16)
            for c in range(PAD)
        ],
        axis=1,
    )
    mine = dot(hot, held[...]).astype(BF16)
    both = dot(mine, twice_ref[...])
    depth = column(depth_ref[...].astype(F32))
    lane = lanes((128, 128))
    mask = jnp.where((lane % 16).astype(F32) < depth, 4.0, 0.0)
    first = lane < 64
    weights = line_weights()
    plane = plane_ref[...]
    for a in range(16):
        low = int(np.flatnonzero(weights[a])[0])
        value = float(weights[a, low]) * both[:, low * 128 : low * 128 + 128] + float(
            weights[a, low + 1]
        ) * both[:, low * 128 + 128 : low * 128 + 256]
        rest = value - value.astype(BF16).astype(F32)
        fine = dot(jnp.where(first, value, rest).astype(BF16), plane)
        for b in range(2):
            at = a * 256 + b * 128
            t = t_ref[:, at : at + 128].astype(F32)
            k = k_ref[:, at : at + 128].astype(F32)
            square = t * t
            out_ref[:, at : at + 128] = k * (
                fine[:, b * 128 : b * 128 + 128] - mask * (square * square)
            )


VM = pl.BlockSpec(memory_space=pltpu.VMEM)
LIMIT = 60 * 1024 * 1024


def struct(*shape):
    return jax.ShapeDtypeStruct(shape, F32)


def call(kernel, out, n_in, scratch=(), collective=None, name=None):
    params = {"vmem_limit_bytes": LIMIT}
    if collective is not None:
        params.update(collective_id=collective, has_side_effects=True)
    several = isinstance(out, (list, tuple))
    return pl.pallas_call(
        kernel,
        out_shape=out,
        in_specs=[VM] * n_in,
        out_specs=[VM] * len(out) if several else VM,
        scratch_shapes=list(scratch),
        compiler_params=pltpu.CompilerParams(**params),
        name=name,
    )


def on_device(thermal_state, opacity_field, glowing_depth, position_to_tile, tile_to_position):
    dma = pltpu.SemaphoreType.DMA
    depth = glowing_depth.reshape(1, SLOTS)
    boxes = position_to_tile.reshape(1, SLOTS)
    places = tile_to_position.reshape(BX, BY, BZ).transpose(1, 0, 2).reshape(1, SLOTS)
    target, source = call(index_kernel, [struct(1, SLOTS), struct(1, SLOTS)], 2, name="index")(
        boxes, places
    )
    steps = SLOTS // ROWS
    wide = pl.BlockSpec((ROWS, 4096), lambda i: (i, 0))
    few = pl.BlockSpec((1, ROWS), lambda i: (0, i))
    outgoing = pl.pallas_call(
        restrict_kernel,
        out_shape=struct(NDEV, CAP, 128),
        grid=(steps,),
        in_specs=[wide, wide, few, VM, VM],
        out_specs=pl.BlockSpec((NDEV, CAP, 128), lambda i: (0, 0, 0)),
        scratch_shapes=[pltpu.VMEM((SLOTS, 128), F32)],
        compiler_params=pltpu.CompilerParams(vmem_limit_bytes=LIMIT),
        name="restrict",
    )(thermal_state, opacity_field, depth, target, average_table())
    arrived = call(
        exchange_kernel, struct(NDEV, CAP, 128), 1, [dma, dma, dma], 0, name="exchange"
    )(outgoing)
    grid = call(assemble_kernel, struct(2, CX, CY, 128), 2, name="assemble")(arrived, source)
    hx, hy, hc = call(
        halo_kernel,
        [struct(2, 2, XH, CY, 128), struct(2, 2, CX, YH, 128), struct(4, 2, XH, YH, 128)],
        1,
        [dma((8,)), dma((8,))],
        1,
        name="halo",
    )(grid)
    plane = struct(CX + 2, EY, 128)
    a, b, c, low = call(
        solve_kernel,
        [plane, plane, plane, struct(1, 128)],
        4,
        [
            pltpu.VMEM((2, EX, EY, 128), F32),
            pltpu.VMEM((6, EX, EY, 128), F32),
            pltpu.VMEM((5, EX, EY, 128), F32),
        ],
        name="solve",
    )(grid, hx, hy, hc)
    lows = call(lowest_kernel, struct(NDEV, 1, 128), 1, [dma, dma, dma], 2, name="lowest")(low)
    leaving = call(
        pack_kernel,
        struct(NDEV, 2, CAP, 128),
        6,
        [pltpu.VMEM((CX + 2, EY, 128), F32), pltpu.VMEM((2, SLOTS, 256), BF16)],
        name="pack",
    )(a, b, c, lows, source, select_table())
    back = call(
        exchange_kernel, struct(NDEV, 2, CAP, 128), 1, [dma, dma, dma], 3, name="return"
    )(leaving)
    return pl.pallas_call(
        prolong_kernel,
        out_shape=struct(SLOTS, 4096),
        grid=(steps,),
        in_specs=[VM, few, wide, wide, few, VM, VM],
        out_specs=wide,
        scratch_shapes=[pltpu.VMEM((NDEV * PAD, 512), BF16)],
        compiler_params=pltpu.CompilerParams(vmem_limit_bytes=LIMIT),
        name="prolong",
    )(back, target, thermal_state, opacity_field, depth, twice_table(), plane_table())


def solution(mesh):
    rows = P(("gx", "gy"), None)
    ints = P(("gx", "gy"))
    return jax.shard_map(
        on_device,
        mesh=mesh,
        in_specs=(rows, rows, ints, ints, ints),
        out_specs=rows,
        check_vma=False,
    )
```

```python
import jax
import jax.numpy as jnp
import numpy as np
from jax import lax
from jax.experimental import pallas as pl
from jax.experimental.pallas import tpu as pltpu
from jax.sharding import PartitionSpec as P

MESH = pl.DeviceIdType.MESH
F32 = jnp.float32
BF16 = jnp.bfloat16
BX, BY, BZ = 4, 6, 32
CX, CY = 16, 24
SLOTS = 768
NDEV = 128
CAP = 12
PAD = 16
ROWS = 128
XH, YH = 6, 8
EX, EY = CX + 2 * XH, CY + 2 * YH


def average_table():
    table = np.zeros((4, 2, 2, 8, 16, 4, 2, 4, 4), np.float32)
    for i in range(4):
        for bh in range(2):
            for f in range(2):
                for b in range(8):
                    for c in range(16):
                        table[i, bh, f, b, c, c // 4, f, i, 2 * bh + b // 4] = 1.0 / 64.0
    return jnp.asarray(table.reshape(8, 256, 128), BF16)


def select_table():
    table = np.zeros((BY, 6, 128, 128), np.float32)
    for v in range(BY):
        for l in range(6):
            for i in range(3):
                for j in range(6):
                    table[v, l, i * 40 + 7 + 4 * v + j, i * 42 + j * 6 + l] = 1.0
    return jnp.asarray(table.reshape(BY, 768, 128), BF16)


def twice_table():
    table = np.zeros((2, 2, 128, 6, 2, 64), np.float32)
    for i in range(6):
        for jl in range(36):
            table[:, i // 3, (i % 3) * 42 + jl, i, :, jl] = 1.0
    return jnp.asarray(table.reshape(512, 768), BF16)


def line_weights():
    weights = np.zeros((16, 6))
    for a in range(16):
        position = (a + 0.5) / 4 + 0.5
        low = int(np.floor(position))
        weights[a, low] += 1.0 - (position - low)
        weights[a, low + 1] += position - low
    return weights


def plane_table():
    w = line_weights()
    plane = np.zeros((2, 64, 256))
    plane[:, :36] = np.kron(w, w).T
    return jnp.asarray(plane.reshape(128, 256), BF16)


def halves(x):
    high = x.astype(BF16)
    return high, (x - high.astype(F32)).astype(BF16)


def dot(a, b):
    return jnp.dot(a, b, preferred_element_type=F32)


def column(row):
    return jnp.broadcast_to(row, (128, 128)).T


def lanes(shape):
    return lax.broadcasted_iota(jnp.int32, shape, len(shape) - 1)


def flipped(x, k):
    return (x, x + 1 - 2 * (x % 2), (x + 2) % 4, 3 - x)[k]


def hops(q):
    near = (0, 1, 2, 1)
    return near[q // 32] + near[q // 8 % 4] + near[q // 2 % 4]


def peer_ids():
    gx, gy = lax.axis_index("gx"), lax.axis_index("gy")
    xs = [flipped(gx // 4, k) * 4 for k in range(4)]
    ys = [flipped(gx % 4, k) for k in range(4)]
    zs = [flipped(gy // 2, k) * 2 for k in range(4)]
    cs = [gy % 2, 1 - gy % 2]
    return [(xs[q // 32] + ys[q // 8 % 4], zs[q // 2 % 4] + cs[q % 2]) for q in range(NDEV)]


CHUNKS = sorted(range(8), key=lambda c: -sum(hops(16 * c + t) for t in range(16)))


def chunk_peers(c):
    return sorted((q for q in range(16 * c, 16 * c + 16) if q), key=lambda q: -hops(q))


def remote(src, dst, send_sem, recv_sem, who):
    return pltpu.make_async_remote_copy(
        src_ref=src,
        dst_ref=dst,
        send_sem=send_sem,
        recv_sem=recv_sem,
        device_id=who,
        device_id_type=MESH,
    )


def rank_row(owner, key):
    owner_c = [column(owner[:, i * 128 : i * 128 + 128]) for i in range(6)]
    key_c = [column(key[:, i * 128 : i * 128 + 128]) for i in range(6)]
    out = []
    for j in range(6):
        ro, rk = owner[:, j * 128 : j * 128 + 128], key[:, j * 128 : j * 128 + 128]
        total = jnp.zeros((128, 128), F32)
        for i in range(6):
            total += jnp.where((owner_c[i] == ro) & (key_c[i] < rk), 1.0, 0.0)
        out.append(jnp.sum(total, axis=0, keepdims=True))
    return jnp.concatenate(out, axis=1)


def target_of(box):
    box = box.astype(F32)
    owner = jnp.floor((box + 0.5) * (1.0 / SLOTS))
    return owner * PAD + rank_row(owner, lanes((1, SLOTS)).astype(F32))


def source_of(slot):
    slot = slot.astype(F32)
    home = jnp.floor((slot + 0.5) * (1.0 / SLOTS))
    rows = home * PAD + rank_row(home, slot)
    group = lanes((1, 128)) // 32
    out = []
    for v in range(BY):
        mixed = None
        for u in range(BX):
            at = u * BY + v
            part = rows[:, at // 4 * 128 : at // 4 * 128 + 128]
            part = pltpu.roll(part, (u - at) * 32 % 128, 1)
            mixed = part if mixed is None else jnp.where(group == u, part, mixed)
        out.append(mixed)
    return jnp.concatenate(out, axis=1)


def one_hot(row, start, me):
    index = lax.broadcasted_iota(jnp.int32, (256, SLOTS), 0) + start
    index = jnp.bitwise_xor(index, jnp.broadcast_to(me * PAD, (256, SLOTS)))
    return jnp.where(index.astype(F32) == row, 1.0, 0.0).astype(BF16)


def restrict_block(step, t_ref, k_ref, depths, table_ref, glow_ref, held):
    at_row = pl.ds(pl.multiple_of(step * ROWS, ROWS), ROWS)
    depth = column(depths[pl.ds(step, 1), :])
    layer = (lanes((ROWS, 128)) % 16).astype(F32)
    mask = jnp.where(layer < depth, 4.0, 0.0)
    total = jnp.zeros((ROWS, 128), F32)
    for i in range(4):
        for bh in range(2):
            glow = absorb = None
            for a in range(4):
                at = (4 * i + a) * 256 + bh * 128
                t = t_ref[at_row, at : at + 128].astype(F32)
                k = k_ref[at_row, at : at + 128].astype(F32)
                square = t * t
                term = k * (square * square) * mask
                glow_ref[at_row, at : at + 128] = term
                glow = term if glow is None else glow + term
                absorb = k if absorb is None else absorb + k
            high, low = halves(jnp.concatenate([glow, absorb], axis=1))
            table = table_ref[2 * i + bh]
            total += dot(high, table) + dot(low, table)
    held[at_row, :] = total


def send_out(x_ref, make_block, put, o_ref, send_sem, recv_sems):
    ids = peer_ids()
    before = None
    for n, c in enumerate(CHUNKS + [None]):
        if c is not None:
            put(c, make_block(c))
        if before is not None:
            for q in chunk_peers(before):
                remote(x_ref.at[q], o_ref.at[q], send_sem, recv_sems.at[before], ids[q]).start()
        before = c
    o_ref[0] = x_ref[0]


def chunk_of(c):
    return pl.ds(1, 15) if c == 0 else pl.ds(16 * c, 16)


def padded_rows(value):
    n = value.shape[0]
    zeros = jnp.zeros((n, PAD - CAP, 128), F32)
    return jnp.concatenate([value, zeros], axis=1).reshape(n * PAD, 128)


def assemble(arrived, recv_sems, source, me, grid_ref):
    total = jnp.zeros((128, SLOTS), F32)
    for c in CHUNKS:
        pltpu.make_async_copy(
            arrived.at[chunk_of(c)], arrived.at[chunk_of(c)], recv_sems.at[c]
        ).wait()
        rows = padded_rows(arrived[16 * c : 16 * c + 16])
        high, low = halves(jnp.concatenate([rows[:128].T, rows[128:].T], axis=1))
        hot = one_hot(source, c * 256, me)
        total += dot(high, hot) + dot(low, hot)
    group = lanes((32, 128)) // 32
    for v in range(BY):
        for u in range(BX):
            out = None
            for l in range(4):
                part = total[l * 32 : l * 32 + 32, v * 128 : v * 128 + 128]
                part = pltpu.roll(part, (l - u) * 32 % 128, 1)
                out = part if out is None else jnp.where(group == l, part, out)
            for f in range(2):
                for i in range(4):
                    at = (f * 4 + i) * 4
                    grid_ref[f, 4 * u + i, 4 * v : 4 * v + 4, :] = out[at : at + 4]


def halo_copies(f, grid_ref, hx_ref, hy_ref, hc_ref, send_sem, recv_sem):
    gx, gy = lax.axis_index("gx"), lax.axis_index("gy")
    up_x, down_x = (gx + 1) % 16, (gx + 15) % 16
    up_y, down_y = (gy + 1) % 8, (gy + 7) % 8
    last_x, first_x = pl.ds(CX - XH, XH), pl.ds(0, XH)
    last_y, first_y = pl.ds(CY - YH, YH), pl.ds(0, YH)
    plan = [
        (grid_ref.at[f, last_x, last_y], hc_ref.at[f, 0], (up_x, up_y)),
        (grid_ref.at[f, last_x, first_y], hc_ref.at[f, 1], (up_x, down_y)),
        (grid_ref.at[f, first_x, last_y], hc_ref.at[f, 2], (down_x, up_y)),
        (grid_ref.at[f, first_x, first_y], hc_ref.at[f, 3], (down_x, down_y)),
        (grid_ref.at[f, last_x], hx_ref.at[f, 0], (up_x, gy)),
        (grid_ref.at[f, first_x], hx_ref.at[f, 1], (down_x, gy)),
        (grid_ref.at[f, :, last_y], hy_ref.at[f, 0], (gx, up_y)),
        (grid_ref.at[f, :, first_y], hy_ref.at[f, 1], (gx, down_y)),
    ]
    return [
        remote(src, dst, send_sem.at[f, n], recv_sem.at[f, n], who)
        for n, (src, dst, who) in enumerate(plan)
    ]


def spread_halo(f, ext, hx_ref, hy_ref, hc_ref):
    own_x, own_y = pl.ds(XH, CX), pl.ds(YH, CY)
    for side, at in ((0, 0), (1, XH + CX)):
        ext[f, pl.ds(at, XH), own_y] = hx_ref[f, side]
    for side, at in ((0, 0), (1, YH + CY)):
        ext[f, own_x, pl.ds(at, YH)] = hy_ref[f, side]
    for n, (atx, aty) in enumerate(
        ((0, 0), (0, YH + CY), (XH + CX, 0), (XH + CX, YH + CY))
    ):
        ext[f, pl.ds(atx, XH), pl.ds(aty, YH)] = hc_ref[f, n]


def z_lower(v):
    lane = lanes(v.shape)
    return jnp.where(lane < 32, pltpu.roll(v, 33, 1), pltpu.roll(v, 32, 1))


def z_upper(v):
    lane = lanes(v.shape)
    return jnp.where(lane >= 96, pltpu.roll(v, 95, 1), pltpu.roll(v, 96, 1))


def face(a, b):
    return (2.0 / 3.0) / (a + b)


def coefficients(ext, w):
    gx, gy = lax.axis_index("gx"), lax.axis_index("gy")
    shape = (EY, 128)
    row = lax.broadcasted_iota(jnp.int32, shape, 0)
    lane = lanes(shape)
    y_at = gy * CY + row - YH
    has_ym, has_yp = y_at >= 1, y_at <= 8 * CY - 2
    has_zm, has_zp = lane != 0, lane != 127

    def plane(x, low):
        x_at = gx * CX + x - XH
        k = ext[1, x]
        has_xm = jnp.broadcast_to(x_at, shape) >= 1
        has_xp = jnp.broadcast_to(x_at, shape) <= 16 * CX - 2
        near = (
            (has_xm, ext[1, x - 1]),
            (has_xp, ext[1, x + 1]),
            (has_ym, pltpu.roll(k, 1, 0)),
            (has_yp, pltpu.roll(k, EY - 1, 0)),
            (has_zm, z_lower(k)),
            (has_zp, z_upper(k)),
        )
        faces = [face(k, jnp.where(has, other, k)) for has, other in near]
        diagonal = k
        for c in faces:
            diagonal = diagonal + c
        inverse = 1.0 / diagonal
        for n, c in enumerate(faces):
            w[n, x] = jnp.where(near[n][0], c * inverse, 0.0)
        w[6, x] = inverse
        own = jnp.broadcast_to((x >= XH) & (x < XH + CX), shape)
        return jnp.minimum(low, jnp.where(own, k * inverse, 1.0))

    def pair(n, low):
        return plane(2 + 2 * n, plane(1 + 2 * n, low))

    low = lax.fori_loop(0, (EX - 2) // 2, pair, jnp.ones(shape, F32))
    low = jnp.min(low[YH : YH + CY], axis=0, keepdims=True)
    return jnp.min(low, axis=1, keepdims=True)


def powers(ext, w, v):
    for x in range(1, EX - 1):
        v[0, x] = w[6, x] * ext[0, x]
    for n, width in enumerate((4, 2, 4, 3)):
        count = (EX - 4 - 2 * n) // width

        def several(m, _, n=n, width=width):
            for t in range(width):
                x = 2 + n + m * width + t
                mid = v[n, x]
                v[n + 1, x] = (
                    w[0, x] * v[n, x - 1]
                    + w[1, x] * v[n, x + 1]
                    + w[2, x] * pltpu.roll(mid, 1, 0)
                    + w[3, x] * pltpu.roll(mid, EY - 1, 0)
                    + w[4, x] * z_lower(mid)
                    + w[5, x] * z_upper(mid)
                )
            return 0

        lax.fori_loop(0, count, several, 0)


def incident(v, lows, inc):
    gx, gy = lax.axis_index("gx"), lax.axis_index("gy")
    shape = (EY, 128)
    lowest = jnp.min(lows[...], axis=0)
    delta = 1.0 - jnp.broadcast_to(lowest, shape)
    square = delta * delta
    scale = 1.0 / (16.0 - 20.0 * square + 5.0 * square * square)
    outer = 16.0 * scale
    inner = outer - 20.0 * square * scale
    row = lax.broadcasted_iota(jnp.int32, shape, 0)
    first_row = (row == YH - 1) & jnp.broadcast_to(gy == 0, shape)
    last_row = (row == YH + CY) & jnp.broadcast_to(gy == 7, shape)
    for x in range(CX + 2):
        at = x + XH - 1
        value = v[0, at] + inner * (v[1, at] + v[2, at]) + outer * (v[3, at] + v[4, at])
        value = jnp.where(first_row, pltpu.roll(value, EY - 1, 0), value)
        inc[x] = jnp.where(last_row, pltpu.roll(value, 1, 0), value)
    inc[0] = jnp.where(jnp.broadcast_to(gx == 0, shape), inc[1], inc[0])
    inc[CX + 1] = jnp.where(jnp.broadcast_to(gx == 15, shape), inc[CX], inc[CX + 1])


def cut_windows(inc, table_ref, win):
    edge = lax.broadcasted_iota(jnp.int32, (32, 128), 0)
    for h in range(2):
        pieces = [[] for _ in range(6)]
        for u in range(BX):
            stack = [inc[4 * u + 3 * h + i] for i in range(3)]
            stack = jnp.concatenate([*stack, jnp.zeros((8, 128), F32)], axis=0).T
            part = [stack[l * 32 : l * 32 + 32] for l in range(4)]
            pieces[0].append(jnp.where(edge == 0, part[0], pltpu.roll(part[3], 1, 0)))
            for l in range(4):
                pieces[l + 1].append(part[l])
            pieces[5].append(jnp.where(edge == 31, part[3], pltpu.roll(part[0], 31, 0)))
        rows = jnp.concatenate([jnp.concatenate(p, axis=0) for p in pieces], axis=1)
        high, low = halves(rows)
        for v in range(BY):
            table = table_ref[v]
            top, rest = halves(dot(high, table) + dot(low, table))
            win[0, v * 128 : v * 128 + 128, h * 128 : h * 128 + 128] = top
            win[1, v * 128 : v * 128 + 128, h * 128 : h * 128 + 128] = rest


def couple_kernel(
    t_hbm, k_hbm, depth_hbm, boxes_hbm, places_hbm, average_hbm, select_hbm,
    back_ref, target_ref, glow_ref, k_ref,
    t_ref, depth_ref, boxes_ref, places_ref, average_ref, select_ref,
    depths, held, source_ref, outgoing, arrived, grid_ref, hx, hy, hc, ext, w, v,
    low_ref, lows, inc, win, leaving,
    t_sem, k_sem, small_sem,
    out_send, out_recv, halo_send, halo_recv, low_send, low_recv, back_send, back_recv,
):
    me = lax.axis_index("gx") * 8 + lax.axis_index("gy")
    barrier = pltpu.get_barrier_semaphore()
    steps = SLOTS // ROWS

    def block_copies(step):
        rows = pl.ds(pl.multiple_of(step * ROWS, ROWS), ROWS)
        return (
            pltpu.make_async_copy(t_hbm.at[rows], t_ref.at[rows], t_sem.at[step]),
            pltpu.make_async_copy(k_hbm.at[rows], k_ref.at[rows], k_sem.at[step]),
        )

    small = [
        pltpu.make_async_copy(src, dst, small_sem.at[n])
        for n, (src, dst) in enumerate(
            (
                (depth_hbm, depth_ref),
                (boxes_hbm, boxes_ref),
                (places_hbm, places_ref),
                (average_hbm, average_ref),
                (select_hbm, select_ref),
            )
        )
    ]
    for copy in small[:4]:
        copy.start()
    for step in range(steps):
        for copy in block_copies(step):
            copy.start()
    small[4].start()
    for who in peer_ids()[1:]:
        pl.semaphore_signal(barrier, inc=1, device_id=who, device_id_type=MESH)
    for copy in small[:4]:
        copy.wait()
    depth = depth_ref[...].astype(F32).reshape(1, SLOTS)
    for n in range(steps):
        depths[n : n + 1, :] = depth[:, n * ROWS : n * ROWS + ROWS]
    target_ref[...] = target_of(boxes_ref[...].reshape(1, SLOTS))
    source_ref[...] = source_of(places_ref[...].reshape(1, SLOTS))

    @pl.loop(0, steps)
    def _(step):
        for copy in block_copies(step):
            copy.wait()
        restrict_block(step, t_ref, k_ref, depths, average_ref, glow_ref, held)

    small[4].wait()
    high, low = halves(held[...])
    target, source = target_ref[...], source_ref[...]
    pl.semaphore_wait(barrier, NDEV - 1)

    def to_owner(c):
        hot = one_hot(target, c * 256, me)
        return dot(hot, high) + dot(hot, low)

    def put_out(c, block):
        outgoing[16 * c : 16 * c + 16] = block.reshape(16, PAD, 128)[:, :CAP]

    send_out(outgoing, to_owner, put_out, arrived, out_send, out_recv)
    assemble(arrived, out_recv, source, me, grid_ref)
    ext[1, pl.ds(XH, CX), pl.ds(YH, CY)] = grid_ref[1]
    copies = [
        halo_copies(f, grid_ref, hx, hy, hc, halo_send, halo_recv) for f in range(2)
    ]
    for f in (1, 0):
        for copy in copies[f]:
            copy.start()
    ext[0, pl.ds(XH, CX), pl.ds(YH, CY)] = grid_ref[0]
    for copy in copies[1]:
        copy.wait()
    spread_halo(1, ext, hx, hy, hc)
    low_ref[...] = jnp.broadcast_to(coefficients(ext, w), (1, 128))
    for copy in copies[0]:
        copy.wait()
    spread_halo(0, ext, hx, hy, hc)
    ids = peer_ids()
    for q in sorted(range(1, NDEV), key=lambda q: -hops(q)):
        remote(low_ref, lows.at[q], low_send, low_recv, ids[q]).start()
    lows[0] = low_ref[...]
    powers(ext, w, v)
    others = pl.ds(1, NDEV - 1)
    pltpu.make_async_copy(lows.at[others], lows.at[others], low_recv).wait()
    incident(v, lows, inc)
    cut_windows(inc, select_ref, win)

    def to_slots(c):
        hot = one_hot(source, c * 256, me)
        return dot(hot, win[0]) + dot(hot, win[1])

    def put_back(c, block):
        for h in range(2):
            part = block[:, h * 128 : h * 128 + 128].reshape(16, PAD, 128)
            leaving[16 * c : 16 * c + 16, h] = part[:, :CAP]

    send_out(leaving, to_slots, put_back, back_ref, back_send, back_recv)
    for c in CHUNKS:
        pltpu.make_async_copy(
            back_ref.at[chunk_of(c)], back_ref.at[chunk_of(c)], back_recv.at[c]
        ).wait()
    pltpu.make_async_copy(lows.at[others], lows.at[others], low_send).wait()
    pltpu.make_async_copy(outgoing.at[others], outgoing.at[others], out_send).wait()
    pltpu.make_async_copy(leaving.at[others], leaving.at[others], back_send).wait()


def prolong_kernel(back_ref, target_ref, k_ref, glow_ref, twice_ref, plane_ref, out_ref, held):
    step = pl.program_id(0)
    me = lax.axis_index("gx") * 8 + lax.axis_index("gy")

    @pl.when(step == 0)
    def _():
        for h in range(2):
            high, low = halves(padded_rows(back_ref[:, h]))
            held[:, h * 128 : h * 128 + 128] = high
            held[:, 256 + h * 128 : 256 + h * 128 + 128] = low

    at_row = pl.ds(pl.multiple_of(step * ROWS, ROWS), ROWS)
    target = column(target_ref[:, at_row])
    place = jnp.bitwise_xor(lanes((ROWS, NDEV * PAD)), jnp.broadcast_to(me * PAD, (ROWS, NDEV * PAD)))
    place = place.astype(F32)
    hot = jnp.concatenate(
        [
            jnp.where(place[:, c * 128 : c * 128 + 128] == target, 1.0, 0.0).astype(BF16)
            for c in range(PAD)
        ],
        axis=1,
    )
    mine = dot(hot, held[...]).astype(BF16)
    both = dot(mine, twice_ref[...])
    first = lanes((ROWS, 128)) < 64
    weights = line_weights()
    plane = plane_ref[...]
    for a in range(16):
        low = int(np.flatnonzero(weights[a])[0])
        value = float(weights[a, low]) * both[:, low * 128 : low * 128 + 128] + float(
            weights[a, low + 1]
        ) * both[:, low * 128 + 128 : low * 128 + 256]
        rest = value - value.astype(BF16).astype(F32)
        fine = dot(jnp.where(first, value, rest).astype(BF16), plane)
        at = slice(a * 256, a * 256 + 256)
        out_ref[:, at] = k_ref[at_row, at].astype(F32) * fine - glow_ref[at_row, at]


VM = pl.BlockSpec(memory_space=pltpu.VMEM)
HB = pl.BlockSpec(memory_space=pltpu.HBM)
MIB = 1024 * 1024


def struct(*shape):
    return jax.ShapeDtypeStruct(shape, F32)


def on_device(thermal_state, opacity_field, glowing_depth, position_to_tile, tile_to_position):
    dma = pltpu.SemaphoreType.DMA
    steps = SLOTS // ROWS
    wide = pl.BlockSpec((ROWS, 4096), lambda i: (i, 0))

    def vmem(*shape, dtype=F32):
        return pltpu.VMEM(shape, dtype)

    back, target, glow, absorb = pl.pallas_call(
        couple_kernel,
        out_shape=[
            vmem(NDEV, 2, CAP, 128),
            vmem(1, SLOTS),
            vmem(SLOTS, 4096),
            vmem(SLOTS, 4096, dtype=BF16),
        ],
        in_specs=[HB] * 7,
        out_specs=[VM] * 4,
        scratch_shapes=[
            vmem(SLOTS, 4096, dtype=BF16),
            vmem(SLOTS, dtype=jnp.int32),
            vmem(SLOTS, dtype=jnp.int32),
            vmem(SLOTS, dtype=jnp.int32),
            vmem(8, 256, 128, dtype=BF16),
            vmem(BY, 768, 128, dtype=BF16),
            vmem(8, 128),
            vmem(SLOTS, 128),
            vmem(1, SLOTS),
            vmem(NDEV, CAP, 128),
            vmem(NDEV, CAP, 128),
            vmem(2, CX, CY, 128),
            vmem(2, 2, XH, CY, 128),
            vmem(2, 2, CX, YH, 128),
            vmem(2, 4, XH, YH, 128),
            vmem(2, EX, EY, 128),
            vmem(7, EX, EY, 128),
            vmem(5, EX, EY, 128),
            vmem(1, 128),
            vmem(NDEV, 1, 128),
            vmem(CX + 2, EY, 128),
            vmem(2, SLOTS, 256, dtype=BF16),
            vmem(NDEV, 2, CAP, 128),
            dma((steps,)),
            dma((steps,)),
            dma((5,)),
            dma,
            dma((8,)),
            dma((2, 8)),
            dma((2, 8)),
            dma,
            dma,
            dma,
            dma((8,)),
        ],
        compiler_params=pltpu.CompilerParams(
            collective_id=0, has_side_effects=True, vmem_limit_bytes=30 * MIB
        ),
        name="couple",
    )(
        *(
            pltpu.with_memory_space_constraint(x, pltpu.HBM)
            for x in (
                thermal_state,
                opacity_field,
                glowing_depth,
                position_to_tile,
                tile_to_position,
                average_table(),
                select_table(),
            )
        )
    )
    return pl.pallas_call(
        prolong_kernel,
        out_shape=struct(SLOTS, 4096),
        grid=(steps,),
        in_specs=[VM, VM, VM, VM, VM, VM],
        out_specs=wide,
        scratch_shapes=[pltpu.VMEM((NDEV * PAD, 512), BF16)],
        compiler_params=pltpu.CompilerParams(vmem_limit_bytes=20 * MIB),
        name="prolong",
    )(
        *(pltpu.with_memory_space_constraint(x, pltpu.VMEM) for x in (back, target, absorb, glow)),
        twice_table(),
        plane_table(),
    )


def solution(mesh):
    rows = P(("gx", "gy"), None)
    ints = P(("gx", "gy"))
    return jax.shard_map(
        on_device,
        mesh=mesh,
        in_specs=(rows, rows, ints, ints, ints),
        out_specs=rows,
        check_vma=False,
    )
```

```python
import jax
import jax.numpy as jnp
import numpy as np
from jax import lax
from jax.experimental import pallas as pl
from jax.experimental.pallas import tpu as pltpu
from jax.sharding import PartitionSpec as P

MESH = pl.DeviceIdType.MESH
F32 = jnp.float32
BF16 = jnp.bfloat16
BX, BY, BZ = 4, 6, 32
CX, CY = 16, 24
SLOTS = 768
NDEV = 128
CAP = 12
PAD = 16
ROWS = 128
XH, YH = 6, 8
EX, EY = CX + 2 * XH, CY + 2 * YH


def average_table():
    table = np.zeros((4, 2, 2, 8, 16, 4, 2, 4, 4), np.float32)
    for i in range(4):
        for bh in range(2):
            for f in range(2):
                for b in range(8):
                    for c in range(16):
                        table[i, bh, f, b, c, c // 4, f, i, 2 * bh + b // 4] = 1.0 / 64.0
    return jnp.asarray(table.reshape(8, 256, 128), BF16)


def select_table():
    table = np.zeros((6, 128, 128), np.float32)
    for l in range(6):
        for i in range(3):
            for j in range(6):
                table[l, i * 40 + 7 + j, i * 42 + j * 6 + l] = 1.0
    return jnp.asarray(table, BF16)


def twice_table():
    table = np.zeros((2, 2, 128, 6, 2, 64), np.float32)
    for i in range(6):
        for jl in range(36):
            table[:, i // 3, (i % 3) * 42 + jl, i, :, jl] = 1.0
    return jnp.asarray(table.reshape(512, 768), BF16)


def line_weights():
    weights = np.zeros((16, 6))
    for a in range(16):
        position = (a + 0.5) / 4 + 0.5
        low = int(np.floor(position))
        weights[a, low] += 1.0 - (position - low)
        weights[a, low + 1] += position - low
    return weights


def plane_table():
    w = line_weights()
    plane = np.zeros((2, 64, 256))
    plane[:, :36] = np.kron(w, w).T
    return jnp.asarray(plane.reshape(128, 256), BF16)


def halves(x):
    high = x.astype(BF16)
    return high, (x - high.astype(F32)).astype(BF16)


def dot(a, b):
    return jnp.dot(a, b, preferred_element_type=F32)


def column(row):
    return jnp.broadcast_to(row, (128, 128)).T


def lanes(shape):
    return lax.broadcasted_iota(jnp.int32, shape, len(shape) - 1)


def flipped(x, k):
    return (x, x + 1 - 2 * (x % 2), (x + 2) % 4, 3 - x)[k]


def hops(q):
    near = (0, 1, 2, 1)
    return near[q // 32] + near[q // 8 % 4] + near[q // 2 % 4]


def peer_ids():
    gx, gy = lax.axis_index("gx"), lax.axis_index("gy")
    xs = [flipped(gx // 4, k) * 4 for k in range(4)]
    ys = [flipped(gx % 4, k) for k in range(4)]
    zs = [flipped(gy // 2, k) * 2 for k in range(4)]
    cs = [gy % 2, 1 - gy % 2]
    return [(xs[q // 32] + ys[q // 8 % 4], zs[q // 2 % 4] + cs[q % 2]) for q in range(NDEV)]


CHUNKS = range(8)


def peer_of(block):
    t = block % 16
    return t * 8 + (block // 16 ^ t % 8)


def chunk_blocks(c):
    return sorted(
        (n for n in range(16 * c, 16 * c + 16) if n), key=lambda n: -hops(peer_of(n))
    )


def place_index(shape, dim, me, start=0):
    row = lax.broadcasted_iota(jnp.int32, shape, dim) + start
    t = row // PAD % 16
    peer = jnp.bitwise_xor(t * 8 + jnp.bitwise_xor(t % 8, row // 256), jnp.broadcast_to(me, shape))
    return peer * PAD + row % PAD


def remote(src, dst, send_sem, recv_sem, who):
    return pltpu.make_async_remote_copy(
        src_ref=src,
        dst_ref=dst,
        send_sem=send_sem,
        recv_sem=recv_sem,
        device_id=who,
        device_id_type=MESH,
    )


def rank_row(owner, key):
    owner_c = [column(owner[:, i * 128 : i * 128 + 128]) for i in range(6)]
    key_c = [column(key[:, i * 128 : i * 128 + 128]) for i in range(6)]
    out = []
    for j in range(6):
        ro, rk = owner[:, j * 128 : j * 128 + 128], key[:, j * 128 : j * 128 + 128]
        total = jnp.zeros((128, 128), F32)
        for i in range(6):
            total += jnp.where((owner_c[i] == ro) & (key_c[i] < rk), 1.0, 0.0)
        out.append(jnp.sum(total, axis=0, keepdims=True))
    return jnp.concatenate(out, axis=1)


def target_of(box):
    box = box.astype(F32)
    owner = jnp.floor((box + 0.5) * (1.0 / SLOTS))
    return owner * PAD + rank_row(owner, lanes((1, SLOTS)).astype(F32))


def source_of(slot):
    slot = slot.astype(F32)
    home = jnp.floor((slot + 0.5) * (1.0 / SLOTS))
    rows = home * PAD + rank_row(home, slot)
    group = lanes((1, 128)) // 32
    out = []
    for v in range(BY):
        mixed = None
        for u in range(BX):
            at = u * BY + v
            part = rows[:, at // 4 * 128 : at // 4 * 128 + 128]
            part = pltpu.roll(part, (u - at) * 32 % 128, 1)
            mixed = part if mixed is None else jnp.where(group == u, part, mixed)
        out.append(mixed)
    return jnp.concatenate(out, axis=1)


def one_hot(row, base, c):
    index = jnp.bitwise_xor(base, c * PAD).astype(F32)
    return jnp.concatenate(
        [
            jnp.where(index == row[:, n * 128 : n * 128 + 128], 1.0, 0.0).astype(BF16)
            for n in range(SLOTS // 128)
        ],
        axis=1,
    )


def restrict_block(step, t_ref, k_ref, depths, table_ref, glow_ref, held):
    at_row = pl.ds(pl.multiple_of(step * ROWS, ROWS), ROWS)
    depth = column(depths[pl.ds(step, 1), :])
    layer = (lanes((ROWS, 128)) % 16).astype(F32)
    mask = jnp.where(layer < depth, 4.0, 0.0)
    total = jnp.zeros((ROWS, 128), F32)
    for i in range(4):
        for bh in range(2):
            glow = absorb = None
            for a in range(4):
                at = (4 * i + a) * 256 + bh * 128
                t = t_ref[at_row, at : at + 128].astype(F32)
                k = k_ref[at_row, at : at + 128].astype(F32)
                square = t * t
                term = k * (square * square) * mask
                glow_ref[at_row, at : at + 128] = term
                glow = term if glow is None else glow + term
                absorb = k if absorb is None else absorb + k
            high, low = halves(jnp.concatenate([glow, absorb], axis=1))
            table = table_ref[2 * i + bh]
            total += dot(high, table) + dot(low, table)
    held[at_row, :] = total


def send_out(x_ref, make_block, put, o_ref, send_sem, recv_sems):
    ids = peer_ids()
    before = None
    for c in (*CHUNKS, None):
        if c is not None:
            put(c, make_block(c))
        if before is not None:
            for n in chunk_blocks(before):
                remote(
                    x_ref.at[n], o_ref.at[n], send_sem, recv_sems.at[before], ids[peer_of(n)]
                ).start()
        before = c
    o_ref[0] = x_ref[0]


def wait_chunk(o_ref, recv_sems, c):
    blocks = pl.ds(1, 15) if c == 0 else pl.ds(16 * c, 16)
    pltpu.make_async_copy(o_ref.at[blocks], o_ref.at[blocks], recv_sems.at[c]).wait()


def padded_rows(value):
    n = value.shape[0]
    zeros = jnp.zeros((n, PAD - CAP, 128), F32)
    return jnp.concatenate([value, zeros], axis=1).reshape(n * PAD, 128)


def assemble(arrived, recv_sems, source, base, grid_ref):
    total = jnp.zeros((128, SLOTS), F32)
    for c in CHUNKS:
        wait_chunk(arrived, recv_sems, c)
        rows = padded_rows(arrived[16 * c : 16 * c + 16])
        high, low = halves(jnp.concatenate([rows[:128].T, rows[128:].T], axis=1))
        hot = one_hot(source, base, c)
        total += dot(high, hot) + dot(low, hot)
    group = lanes((32, 128)) // 32
    for v in range(BY):
        for u in range(BX):
            out = None
            for l in range(4):
                part = total[l * 32 : l * 32 + 32, v * 128 : v * 128 + 128]
                part = pltpu.roll(part, (l - u) * 32 % 128, 1)
                out = part if out is None else jnp.where(group == l, part, out)
            for f in range(2):
                for i in range(4):
                    at = (f * 4 + i) * 4
                    grid_ref[f, 4 * u + i, 4 * v : 4 * v + 4, :] = out[at : at + 4]


def halo_copies(f, grid_ref, hx_ref, hy_ref, hc_ref, send_sem, recv_sem):
    gx, gy = lax.axis_index("gx"), lax.axis_index("gy")
    up_x, down_x = (gx + 1) % 16, (gx + 15) % 16
    up_y, down_y = (gy + 1) % 8, (gy + 7) % 8
    last_x, first_x = pl.ds(CX - XH, XH), pl.ds(0, XH)
    last_y, first_y = pl.ds(CY - YH, YH), pl.ds(0, YH)
    plan = [
        (grid_ref.at[f, last_x, last_y], hc_ref.at[f, 0], (up_x, up_y)),
        (grid_ref.at[f, last_x, first_y], hc_ref.at[f, 1], (up_x, down_y)),
        (grid_ref.at[f, first_x, last_y], hc_ref.at[f, 2], (down_x, up_y)),
        (grid_ref.at[f, first_x, first_y], hc_ref.at[f, 3], (down_x, down_y)),
        (grid_ref.at[f, last_x], hx_ref.at[f, 0], (up_x, gy)),
        (grid_ref.at[f, first_x], hx_ref.at[f, 1], (down_x, gy)),
        (grid_ref.at[f, :, last_y], hy_ref.at[f, 0], (gx, up_y)),
        (grid_ref.at[f, :, first_y], hy_ref.at[f, 1], (gx, down_y)),
    ]
    return [
        remote(src, dst, send_sem.at[f, n], recv_sem.at[f, n], who)
        for n, (src, dst, who) in enumerate(plan)
    ]


def spread_halo(f, ext, hx_ref, hy_ref, hc_ref):
    own_x, own_y = pl.ds(XH, CX), pl.ds(YH, CY)
    for side, at in ((0, 0), (1, XH + CX)):
        ext[f, pl.ds(at, XH), own_y] = hx_ref[f, side]
    for side, at in ((0, 0), (1, YH + CY)):
        ext[f, own_x, pl.ds(at, YH)] = hy_ref[f, side]
    for n, (atx, aty) in enumerate(
        ((0, 0), (0, YH + CY), (XH + CX, 0), (XH + CX, YH + CY))
    ):
        ext[f, pl.ds(atx, XH), pl.ds(aty, YH)] = hc_ref[f, n]


def z_lower(v):
    lane = lanes(v.shape)
    return jnp.where(lane < 32, pltpu.roll(v, 33, 1), pltpu.roll(v, 32, 1))


def z_upper(v):
    lane = lanes(v.shape)
    return jnp.where(lane >= 96, pltpu.roll(v, 95, 1), pltpu.roll(v, 96, 1))


def face(a, b):
    return (2.0 / 3.0) / (a + b)


def coefficients(ext, w):
    gx, gy = lax.axis_index("gx"), lax.axis_index("gy")
    shape = (EY, 128)
    row = lax.broadcasted_iota(jnp.int32, shape, 0)
    lane = lanes(shape)
    y_at = gy * CY + row - YH
    has_ym, has_yp = y_at >= 1, y_at <= 8 * CY - 2
    has_zm, has_zp = lane != 0, lane != 127

    def plane(x, low):
        x_at = gx * CX + x - XH
        k = ext[1, x]
        has_xm = jnp.broadcast_to(x_at, shape) >= 1
        has_xp = jnp.broadcast_to(x_at, shape) <= 16 * CX - 2
        near = (
            (has_xm, ext[1, x - 1]),
            (has_xp, ext[1, x + 1]),
            (has_ym, pltpu.roll(k, 1, 0)),
            (has_yp, pltpu.roll(k, EY - 1, 0)),
            (has_zm, z_lower(k)),
            (has_zp, z_upper(k)),
        )
        faces = [face(k, jnp.where(has, other, k)) for has, other in near]
        diagonal = k
        for c in faces:
            diagonal = diagonal + c
        inverse = 1.0 / diagonal
        for n, c in enumerate(faces):
            w[n, x] = jnp.where(near[n][0], c * inverse, 0.0)
        w[6, x] = inverse
        own = jnp.broadcast_to((x >= XH) & (x < XH + CX), shape)
        return jnp.minimum(low, jnp.where(own, k * inverse, 1.0))

    def pair(n, low):
        return plane(2 + 2 * n, plane(1 + 2 * n, low))

    low = lax.fori_loop(0, (EX - 2) // 2, pair, jnp.ones(shape, F32))
    low = jnp.min(low[YH : YH + CY], axis=0, keepdims=True)
    return jnp.min(low, axis=1, keepdims=True)


def powers(ext, w, v):
    for x in range(1, EX - 1):
        v[0, x] = w[6, x] * ext[0, x]
    for n, width in enumerate((4, 2, 4, 3)):
        count = (EX - 4 - 2 * n) // width

        def several(m, _, n=n, width=width):
            for t in range(width):
                x = 2 + n + m * width + t
                mid = v[n, x]
                v[n + 1, x] = (
                    w[0, x] * v[n, x - 1]
                    + w[1, x] * v[n, x + 1]
                    + w[2, x] * pltpu.roll(mid, 1, 0)
                    + w[3, x] * pltpu.roll(mid, EY - 1, 0)
                    + w[4, x] * z_lower(mid)
                    + w[5, x] * z_upper(mid)
                )
            return 0

        lax.fori_loop(0, count, several, 0)


def incident(v, lows, inc):
    gx, gy = lax.axis_index("gx"), lax.axis_index("gy")
    shape = (EY, 128)
    lowest = jnp.min(lows[...], axis=0)
    delta = 1.0 - jnp.broadcast_to(lowest, shape)
    square = delta * delta
    scale = 1.0 / (16.0 - 20.0 * square + 5.0 * square * square)
    outer = 16.0 * scale
    inner = outer - 20.0 * square * scale
    row = lax.broadcasted_iota(jnp.int32, shape, 0)
    first_row = (row == YH - 1) & jnp.broadcast_to(gy == 0, shape)
    last_row = (row == YH + CY) & jnp.broadcast_to(gy == 7, shape)
    for x in range(CX + 2):
        at = x + XH - 1
        value = v[0, at] + inner * (v[1, at] + v[2, at]) + outer * (v[3, at] + v[4, at])
        value = jnp.where(first_row, pltpu.roll(value, EY - 1, 0), value)
        inc[x] = jnp.where(last_row, pltpu.roll(value, 1, 0), value)
    inc[0] = jnp.where(jnp.broadcast_to(gx == 0, shape), inc[1], inc[0])
    inc[CX + 1] = jnp.where(jnp.broadcast_to(gx == 15, shape), inc[CX], inc[CX + 1])


def cut_windows(inc, table_ref, win):
    edge = lax.broadcasted_iota(jnp.int32, (32, 128), 0)
    for h in range(2):
        pieces = [[] for _ in range(6)]
        for u in range(BX):
            stack = [inc[4 * u + 3 * h + i] for i in range(3)]
            stack = jnp.concatenate([*stack, jnp.zeros((8, 128), F32)], axis=0).T
            part = [stack[l * 32 : l * 32 + 32] for l in range(4)]
            pieces[0].append(jnp.where(edge == 0, part[0], pltpu.roll(part[3], 1, 0)))
            for l in range(4):
                pieces[l + 1].append(part[l])
            pieces[5].append(jnp.where(edge == 31, part[3], pltpu.roll(part[0], 31, 0)))
        rows = jnp.concatenate([jnp.concatenate(p, axis=0) for p in pieces], axis=1)
        high, low = halves(rows)
        for v in range(BY):
            table = table_ref[v]
            top, rest = halves(dot(high, table) + dot(low, table))
            win[0, v * 128 : v * 128 + 128, h * 128 : h * 128 + 128] = top
            win[1, v * 128 : v * 128 + 128, h * 128 : h * 128 + 128] = rest


def couple_kernel(
    t_hbm, k_hbm, depth_hbm, boxes_hbm, places_hbm, average_hbm, select_hbm,
    mine_ref, glow_ref, k_ref,
    t_ref, depth_ref, boxes_ref, places_ref, average_ref, first_ref, select_ref,
    back_ref, target_ref, target_c, depths, held, source_ref, outgoing, arrived, grid_ref, hx, hy, hc, ext, w, v,
    low_ref, lows, inc, win, leaving,
    t_sem, k_sem, small_sem,
    out_send, out_recv, halo_send, halo_recv, low_send, low_recv, back_send, back_recv,
):
    me = lax.axis_index("gx") * 8 + lax.axis_index("gy")
    barrier = pltpu.get_barrier_semaphore()
    steps = SLOTS // ROWS

    def block_copies(step):
        rows = pl.ds(pl.multiple_of(step * ROWS, ROWS), ROWS)
        return (
            pltpu.make_async_copy(t_hbm.at[rows], t_ref.at[rows], t_sem.at[step]),
            pltpu.make_async_copy(k_hbm.at[rows], k_ref.at[rows], k_sem.at[step]),
        )

    small = [
        pltpu.make_async_copy(src, dst, small_sem.at[n])
        for n, (src, dst) in enumerate(
            (
                (depth_hbm, depth_ref),
                (boxes_hbm, boxes_ref),
                (places_hbm, places_ref),
                (average_hbm, average_ref),
                (select_hbm, first_ref),
            )
        )
    ]
    for copy in small[:3]:
        copy.start()
    for copy in (*block_copies(0), small[3], *block_copies(1)):
        copy.start()
    for who in peer_ids()[1:]:
        pl.semaphore_signal(barrier, inc=1, device_id=who, device_id_type=MESH)
    for copy in small[:3]:
        copy.wait()
    depth = depth_ref[...].astype(F32).reshape(1, SLOTS)
    for n in range(steps):
        depths[n : n + 1, :] = depth[:, n * ROWS : n * ROWS + ROWS]
    target_ref[...] = target_of(boxes_ref[...].reshape(1, SLOTS))
    small[3].wait()

    @pl.loop(0, steps)
    def _(step):
        @pl.when(step + 2 < steps)
        def _():
            for copy in block_copies(step + 2):
                copy.start()

        for copy in block_copies(step):
            copy.wait()
        restrict_block(step, t_ref, k_ref, depths, average_ref, glow_ref, held)

    high, low = halves(held[...])
    target = target_ref[...]
    base = place_index((256, 128), 0, me)
    pl.semaphore_wait(barrier, NDEV - 1)

    def to_owner(c):
        hot = one_hot(target, base, c)
        return dot(hot, high) + dot(hot, low)

    def put_out(c, block):
        outgoing[16 * c : 16 * c + 16] = block.reshape(16, PAD, 128)[:, :CAP]

    send_out(outgoing, to_owner, put_out, arrived, out_send, out_recv)
    small[4].start()
    source_ref[...] = source_of(places_ref[...].reshape(1, SLOTS))
    for n in range(steps):
        target_c[n * ROWS : n * ROWS + ROWS, :] = column(target[:, n * ROWS : n * ROWS + ROWS])
    source = source_ref[...]
    small[4].wait()
    for l in range(6):
        table = first_ref[l].astype(F32)
        for v_at in range(BY):
            moved = pltpu.roll(table, 4 * v_at, 0) if v_at else table
            select_ref[v_at, l * 128 : l * 128 + 128] = moved.astype(BF16)
    assemble(arrived, out_recv, source, base, grid_ref)
    ext[1, pl.ds(XH, CX), pl.ds(YH, CY)] = grid_ref[1]
    copies = [
        halo_copies(f, grid_ref, hx, hy, hc, halo_send, halo_recv) for f in range(2)
    ]
    for copy in copies[1]:
        copy.start()
    ext[0, pl.ds(XH, CX), pl.ds(YH, CY)] = grid_ref[0]
    for copy in copies[1]:
        copy.wait_send()
    for copy in copies[0]:
        copy.start()
    for copy in copies[1]:
        copy.wait_recv()
    spread_halo(1, ext, hx, hy, hc)
    low_ref[...] = jnp.broadcast_to(coefficients(ext, w), (1, 128))
    for copy in copies[0][6:]:
        copy.wait()
    ids = peer_ids()
    for q in sorted(range(1, NDEV), key=lambda q: -hops(q)):
        remote(low_ref, lows.at[q], low_send, low_recv, ids[q]).start()
    lows[0] = low_ref[...]
    for copy in copies[0][:6]:
        copy.wait()
    spread_halo(0, ext, hx, hy, hc)
    powers(ext, w, v)
    others = pl.ds(1, NDEV - 1)
    pltpu.make_async_copy(lows.at[others], lows.at[others], low_recv).wait()
    incident(v, lows, inc)
    cut_windows(inc, select_ref, win)

    def to_slots(c):
        hot = one_hot(source, base, c)
        return dot(hot, win[0]) + dot(hot, win[1])

    def put_back(c, block):
        for h in range(2):
            part = block[:, h * 128 : h * 128 + 128].reshape(16, PAD, 128)
            leaving[16 * c : 16 * c + 16, h] = part[:, :CAP]

    send_out(leaving, to_slots, put_back, back_ref, back_send, back_recv)
    across = place_index((1, 256), 1, me)
    for c in CHUNKS:
        wait_chunk(back_ref, back_recv, c)
        parts = [
            halves(padded_rows(back_ref[16 * c : 16 * c + 16, h])) for h in range(2)
        ]
        rows = jnp.concatenate([part[k] for k in range(2) for part in parts], axis=1)
        index = jnp.bitwise_xor(across, c * PAD).astype(F32)
        for n in range(steps):
            at = slice(n * ROWS, n * ROWS + ROWS)
            hot = jnp.concatenate(
                [
                    jnp.where(
                        index[:, m * 128 : m * 128 + 128] == target_c[at, :], 1.0, 0.0
                    ).astype(BF16)
                    for m in range(2)
                ],
                axis=1,
            )
            found = dot(hot, rows).astype(BF16)
            mine_ref[at, :] = found if c == 0 else mine_ref[at, :] + found
    pltpu.make_async_copy(lows.at[others], lows.at[others], low_send).wait()
    pltpu.make_async_copy(outgoing.at[others], outgoing.at[others], out_send).wait()
    pltpu.make_async_copy(leaving.at[others], leaving.at[others], back_send).wait()


def prolong_kernel(mine_ref, k_ref, glow_ref, twice_ref, plane_ref, out_ref):
    step = pl.program_id(0)
    at_row = pl.ds(pl.multiple_of(step * ROWS, ROWS), ROWS)
    both = dot(mine_ref[at_row, :], twice_ref[...])
    first = lanes((ROWS, 128)) < 64
    weights = line_weights()
    plane = plane_ref[...]
    for a in range(16):
        low = int(np.flatnonzero(weights[a])[0])
        value = float(weights[a, low]) * both[:, low * 128 : low * 128 + 128] + float(
            weights[a, low + 1]
        ) * both[:, low * 128 + 128 : low * 128 + 256]
        rest = value - value.astype(BF16).astype(F32)
        fine = dot(jnp.where(first, value, rest).astype(BF16), plane)
        at = slice(a * 256, a * 256 + 256)
        out_ref[:, at] = k_ref[at_row, at].astype(F32) * fine - glow_ref[at_row, at]


VM = pl.BlockSpec(memory_space=pltpu.VMEM)
HB = pl.BlockSpec(memory_space=pltpu.HBM)
MIB = 1024 * 1024


def struct(*shape):
    return jax.ShapeDtypeStruct(shape, F32)


def on_device(thermal_state, opacity_field, glowing_depth, position_to_tile, tile_to_position):
    dma = pltpu.SemaphoreType.DMA
    steps = SLOTS // ROWS
    wide = pl.BlockSpec((ROWS, 4096), lambda i: (i, 0))

    def vmem(*shape, dtype=F32):
        return pltpu.VMEM(shape, dtype)

    mine, glow, absorb = pl.pallas_call(
        couple_kernel,
        out_shape=[
            vmem(SLOTS, 512, dtype=BF16),
            vmem(SLOTS, 4096),
            vmem(SLOTS, 4096, dtype=BF16),
        ],
        in_specs=[HB] * 7,
        out_specs=[VM] * 3,
        scratch_shapes=[
            vmem(SLOTS, 4096, dtype=BF16),
            vmem(SLOTS, dtype=jnp.int32),
            vmem(SLOTS, dtype=jnp.int32),
            vmem(SLOTS, dtype=jnp.int32),
            vmem(8, 256, 128, dtype=BF16),
            vmem(6, 128, 128, dtype=BF16),
            vmem(BY, 768, 128, dtype=BF16),
            vmem(NDEV, 2, CAP, 128),
            vmem(1, SLOTS),
            vmem(SLOTS, 128),
            vmem(8, 128),
            vmem(SLOTS, 128),
            vmem(1, SLOTS),
            vmem(NDEV, CAP, 128),
            vmem(NDEV, CAP, 128),
            vmem(2, CX, CY, 128),
            vmem(2, 2, XH, CY, 128),
            vmem(2, 2, CX, YH, 128),
            vmem(2, 4, XH, YH, 128),
            vmem(2, EX, EY, 128),
            vmem(7, EX, EY, 128),
            vmem(5, EX, EY, 128),
            vmem(1, 128),
            vmem(NDEV, 1, 128),
            vmem(CX + 2, EY, 128),
            vmem(2, SLOTS, 256, dtype=BF16),
            vmem(NDEV, 2, CAP, 128),
            dma((steps,)),
            dma((steps,)),
            dma((5,)),
            dma,
            dma((8,)),
            dma((2, 8)),
            dma((2, 8)),
            dma,
            dma,
            dma,
            dma((8,)),
        ],
        compiler_params=pltpu.CompilerParams(
            collective_id=0, has_side_effects=True, vmem_limit_bytes=30 * MIB
        ),
        name="couple",
    )(
        *(
            pltpu.with_memory_space_constraint(x, pltpu.HBM)
            for x in (
                thermal_state,
                opacity_field,
                glowing_depth,
                position_to_tile,
                tile_to_position,
                average_table(),
                select_table(),
            )
        )
    )
    return pl.pallas_call(
        prolong_kernel,
        out_shape=struct(SLOTS, 4096),
        grid=(steps,),
        in_specs=[VM] * 5,
        out_specs=wide,
        compiler_params=pltpu.CompilerParams(vmem_limit_bytes=20 * MIB),
        name="prolong",
    )(
        *(pltpu.with_memory_space_constraint(x, pltpu.VMEM) for x in (mine, absorb, glow)),
        twice_table(),
        plane_table(),
    )


def solution(mesh):
    rows = P(("gx", "gy"), None)
    ints = P(("gx", "gy"))
    return jax.shard_map(
        on_device,
        mesh=mesh,
        in_specs=(rows, rows, ints, ints, ints),
        out_specs=rows,
        check_vma=False,
    )
```

```python
import jax
import jax.numpy as jnp
import numpy as np
from jax import lax
from jax.experimental import pallas as pl
from jax.experimental.pallas import tpu as pltpu
from jax.sharding import PartitionSpec as P

MESH = pl.DeviceIdType.MESH
F32 = jnp.float32
BF16 = jnp.bfloat16
BX, BY, BZ = 4, 6, 32
CX, CY = 16, 24
SLOTS = 768
NDEV = 128
CAP = 12
PAD = 16
LINES = 21
ROWS = 128
XH, YH = 6, 8
EX, EY = CX + 2 * XH, CY + 2 * YH


def average_table():
    table = np.zeros((4, 2, 2, 8, 16, 4, 2, 4, 4), np.float32)
    for i in range(4):
        for bh in range(2):
            for f in range(2):
                for b in range(8):
                    for c in range(16):
                        table[i, bh, f, b, c, c // 4, f, i, 2 * bh + b // 4] = 1.0 / 64.0
    return jnp.asarray(table.reshape(8, 256, 128), BF16)


def select_keys():
    keys = np.full((8, 256), -100000, np.int32)
    for n in range(216):
        i, j, l = n // 36, n % 36 // 6, n % 6
        keys[i // 3, n] = l * 128 + i % 3 * 40 + 7 + j
    return jnp.asarray(keys)


def twice_table():
    table = np.zeros((2, 256, 6, 2, 64), np.float32)
    for n in range(216):
        table[:, n, n // 36, :, n % 36] = 1.0
    return jnp.asarray(table.reshape(512, 768), BF16)


def line_weights():
    weights = np.zeros((16, 6))
    for a in range(16):
        position = (a + 0.5) / 4 + 0.5
        low = int(np.floor(position))
        weights[a, low] += 1.0 - (position - low)
        weights[a, low + 1] += position - low
    return weights


def plane_table():
    w = line_weights()
    plane = np.zeros((2, 64, 256))
    plane[:, :36] = np.kron(w, w).T
    return jnp.asarray(plane.reshape(128, 256), BF16)


def halves(x):
    high = x.astype(BF16)
    return high, (x - high.astype(F32)).astype(BF16)


def dot(a, b):
    return jnp.dot(a, b, preferred_element_type=F32)


def column(row):
    return jnp.broadcast_to(row, (128, 128)).T


def lanes(shape):
    return lax.broadcasted_iota(jnp.int32, shape, len(shape) - 1)


def flipped(x, k):
    return (x, x + 1 - 2 * (x % 2), (x + 2) % 4, 3 - x)[k]


def hops(q):
    near = (0, 1, 2, 1)
    return near[q // 32] + near[q // 8 % 4] + near[q // 2 % 4]


def peer_ids():
    gx, gy = lax.axis_index("gx"), lax.axis_index("gy")
    xs = [flipped(gx // 4, k) * 4 for k in range(4)]
    ys = [flipped(gx % 4, k) for k in range(4)]
    zs = [flipped(gy // 2, k) * 2 for k in range(4)]
    cs = [gy % 2, 1 - gy % 2]
    return [(xs[q // 32] + ys[q // 8 % 4], zs[q // 2 % 4] + cs[q % 2]) for q in range(NDEV)]


CHUNKS = range(8)


def peer_of(block):
    t = block % 16
    return t * 8 + (block // 16 ^ t % 8)


def chunk_blocks(c):
    return sorted(
        (n for n in range(16 * c, 16 * c + 16) if n), key=lambda n: -hops(peer_of(n))
    )


def place_index(shape, dim, me, start=0):
    row = lax.broadcasted_iota(jnp.int32, shape, dim) + start
    t = row // PAD % 16
    peer = jnp.bitwise_xor(t * 8 + jnp.bitwise_xor(t % 8, row // 256), jnp.broadcast_to(me, shape))
    return peer * PAD + row % PAD


def remote(src, dst, send_sem, recv_sem, who):
    return pltpu.make_async_remote_copy(
        src_ref=src,
        dst_ref=dst,
        send_sem=send_sem,
        recv_sem=recv_sem,
        device_id=who,
        device_id_type=MESH,
    )


def rank_row(owner, key):
    owner_c = [column(owner[:, i * 128 : i * 128 + 128]) for i in range(6)]
    key_c = [column(key[:, i * 128 : i * 128 + 128]) for i in range(6)]
    out = []
    for j in range(6):
        ro, rk = owner[:, j * 128 : j * 128 + 128], key[:, j * 128 : j * 128 + 128]
        total = jnp.zeros((128, 128), F32)
        for i in range(6):
            total += jnp.where((owner_c[i] == ro) & (key_c[i] < rk), 1.0, 0.0)
        out.append(jnp.sum(total, axis=0, keepdims=True))
    return jnp.concatenate(out, axis=1)


def target_of(box):
    box = box.astype(F32)
    owner = jnp.floor((box + 0.5) * (1.0 / SLOTS))
    return owner * PAD + rank_row(owner, lanes((1, SLOTS)).astype(F32))


def source_of(slot):
    slot = slot.astype(F32)
    home = jnp.floor((slot + 0.5) * (1.0 / SLOTS))
    rows = home * PAD + rank_row(home, slot)
    group = lanes((1, 128)) // 32
    out = []
    for v in range(BY):
        mixed = None
        for u in range(BX):
            at = u * BY + v
            part = rows[:, at // 4 * 128 : at // 4 * 128 + 128]
            part = pltpu.roll(part, (u - at) * 32 % 128, 1)
            mixed = part if mixed is None else jnp.where(group == u, part, mixed)
        out.append(mixed)
    return jnp.concatenate(out, axis=1)


def one_hot(row, base, c):
    index = jnp.bitwise_xor(base, c * PAD).astype(F32)
    return jnp.concatenate(
        [
            jnp.where(index == row[:, n * 128 : n * 128 + 128], 1.0, 0.0).astype(BF16)
            for n in range(SLOTS // 128)
        ],
        axis=1,
    )


def restrict_block(step, t_ref, k_ref, depths, table_ref, glow_ref, held):
    at_row = pl.ds(pl.multiple_of(step * ROWS, ROWS), ROWS)
    depth = column(depths[pl.ds(step, 1), :])
    layer = (lanes((ROWS, 128)) % 16).astype(F32)
    mask = jnp.where(layer < depth, 4.0, 0.0)
    total = jnp.zeros((ROWS, 128), F32)
    for i in range(4):
        for bh in range(2):
            glow = absorb = None
            for a in range(4):
                at = (4 * i + a) * 256 + bh * 128
                t = t_ref[step % 3, :, at : at + 128].astype(F32)
                k = k_ref[at_row, at : at + 128].astype(F32)
                square = t * t
                term = k * (square * square) * mask
                glow_ref[at_row, at : at + 128] = term
                glow = term if glow is None else glow + term
                absorb = k if absorb is None else absorb + k
            high, low = halves(jnp.concatenate([glow, absorb], axis=1))
            table = table_ref[2 * i + bh]
            total += dot(high, table) + dot(low, table)
    held[at_row, :] = total


def send_out(x_ref, make_block, put, o_ref, send_sem, recv_sems):
    ids = peer_ids()
    before = None
    for c in (*CHUNKS, None):
        if c is not None:
            put(c, make_block(c))
        if before is not None:
            for n in chunk_blocks(before):
                remote(
                    x_ref.at[n], o_ref.at[n], send_sem, recv_sems.at[before], ids[peer_of(n)]
                ).start()
        before = c
    o_ref[0] = x_ref[0]


def wait_chunk(o_ref, recv_sems, c):
    blocks = pl.ds(1, 15) if c == 0 else pl.ds(16 * c, 16)
    pltpu.make_async_copy(o_ref.at[blocks], o_ref.at[blocks], recv_sems.at[c]).wait()


def padded_rows(value):
    n = value.shape[0]
    zeros = jnp.zeros((n, PAD - CAP, 128), F32)
    return jnp.concatenate([value, zeros], axis=1).reshape(n * PAD, 128)


def assemble(arrived, recv_sems, source, base, grid_ref):
    total = jnp.zeros((128, SLOTS), F32)
    for c in CHUNKS:
        wait_chunk(arrived, recv_sems, c)
        rows = padded_rows(arrived[16 * c : 16 * c + 16])
        high, low = halves(jnp.concatenate([rows[:128].T, rows[128:].T], axis=1))
        hot = one_hot(source, base, c)
        total += dot(high, hot) + dot(low, hot)
    group = lanes((32, 128)) // 32
    for v in range(BY):
        for u in range(BX):
            out = None
            for l in range(4):
                part = total[l * 32 : l * 32 + 32, v * 128 : v * 128 + 128]
                part = pltpu.roll(part, (l - u) * 32 % 128, 1)
                out = part if out is None else jnp.where(group == l, part, out)
            for f in range(2):
                for i in range(4):
                    at = (f * 4 + i) * 4
                    grid_ref[f, 4 * u + i, 4 * v : 4 * v + 4, :] = out[at : at + 4]


def halo_copies(f, grid_ref, hx_ref, hy_ref, hc_ref, send_sem, recv_sem):
    gx, gy = lax.axis_index("gx"), lax.axis_index("gy")
    up_x, down_x = (gx + 1) % 16, (gx + 15) % 16
    up_y, down_y = (gy + 1) % 8, (gy + 7) % 8
    last_y, first_y = pl.ds(CY - YH, YH), pl.ds(0, YH)
    deep = XH if f else XH - 1
    low, high = pl.ds(XH - deep, deep), pl.ds(0, deep)
    sent_low, sent_high = pl.ds(CX - deep, deep), pl.ds(0, deep)
    plan = [
        (grid_ref.at[f, :, last_y], hy_ref.at[f, 0], (gx, up_y)),
        (grid_ref.at[f, :, first_y], hy_ref.at[f, 1], (gx, down_y)),
        (grid_ref.at[f, sent_low, last_y], hc_ref.at[f, 0, low], (up_x, up_y)),
        (grid_ref.at[f, sent_low, first_y], hc_ref.at[f, 1, low], (up_x, down_y)),
        (grid_ref.at[f, sent_high, last_y], hc_ref.at[f, 2, high], (down_x, up_y)),
        (grid_ref.at[f, sent_high, first_y], hc_ref.at[f, 3, high], (down_x, down_y)),
    ]
    if f:
        near = [
            (grid_ref.at[f, pl.ds(CX - 1, 1)], hx_ref.at[f, 0, pl.ds(XH - 1, 1)], (up_x, gy)),
            (grid_ref.at[f, pl.ds(0, 1)], hx_ref.at[f, 1, pl.ds(0, 1)], (down_x, gy)),
        ]
        far = [
            (grid_ref.at[f, pl.ds(CX - XH, XH - 1)], hx_ref.at[f, 0, pl.ds(0, XH - 1)], (up_x, gy)),
            (grid_ref.at[f, pl.ds(1, XH - 1)], hx_ref.at[f, 1, pl.ds(1, XH - 1)], (down_x, gy)),
        ]
        plan = near + plan[:2] + far + plan[2:]
    else:
        plan = plan + [
            (grid_ref.at[f, sent_low], hx_ref.at[f, 0, low], (up_x, gy)),
            (grid_ref.at[f, sent_high], hx_ref.at[f, 1, high], (down_x, gy)),
        ]
    return [
        remote(src, dst, send_sem.at[f, n], recv_sem.at[f, n], who)
        for n, (src, dst, who) in enumerate(plan)
    ]


def spread_y(f, ext, hy_ref):
    for side, at in ((0, 0), (1, YH + CY)):
        ext[f, pl.ds(XH, CX), pl.ds(at, YH)] = hy_ref[f, side]


def spread_near(ext, hx_ref):
    own_y = pl.ds(YH, CY)
    ext[1, XH - 1, own_y] = hx_ref[1, 0, XH - 1]
    ext[1, XH + CX, own_y] = hx_ref[1, 1, 0]


def spread_x(f, ext, hx_ref, hc_ref):
    deep = XH if f else XH - 1
    for side, skip, at in ((0, XH - deep, XH - deep), (1, 0, XH + CX)):
        planes, from_planes = pl.ds(at, deep), pl.ds(skip, deep)
        ext[f, planes, pl.ds(YH, CY)] = hx_ref[f, side, from_planes]
        ext[f, planes, pl.ds(0, YH)] = hc_ref[f, 2 * side, from_planes]
        ext[f, planes, pl.ds(YH + CY, YH)] = hc_ref[f, 2 * side + 1, from_planes]


def z_lower(v):
    lane = lanes(v.shape)
    return jnp.where(lane < 32, pltpu.roll(v, 33, 1), pltpu.roll(v, 32, 1))


def z_upper(v):
    lane = lanes(v.shape)
    return jnp.where(lane >= 96, pltpu.roll(v, 95, 1), pltpu.roll(v, 96, 1))


def face(a, b):
    return (2.0 / 3.0) / (a + b)


def plane_coefficients(ext, w):
    gx, gy = lax.axis_index("gx"), lax.axis_index("gy")
    shape = (EY, 128)
    row = lax.broadcasted_iota(jnp.int32, shape, 0)
    lane = lanes(shape)
    y_at = gy * CY + row - YH
    has_ym, has_yp = y_at >= 1, y_at <= 8 * CY - 2
    has_zm, has_zp = lane != 0, lane != 127

    def plane(x, low):
        x_at = gx * CX + x - XH
        k = ext[1, x]
        has_xm = jnp.broadcast_to(x_at, shape) >= 1
        has_xp = jnp.broadcast_to(x_at, shape) <= 16 * CX - 2
        near = (
            (has_xm, ext[1, x - 1]),
            (has_xp, ext[1, x + 1]),
            (has_ym, pltpu.roll(k, 1, 0)),
            (has_yp, pltpu.roll(k, EY - 1, 0)),
            (has_zm, z_lower(k)),
            (has_zp, z_upper(k)),
        )
        faces = [face(k, jnp.where(has, other, k)) for has, other in near]
        diagonal = k
        for c in faces:
            diagonal = diagonal + c
        inverse = 1.0 / diagonal
        for n, c in enumerate(faces):
            w[n, x] = jnp.where(near[n][0], c * inverse, 0.0)
        w[6, x] = inverse
        own = jnp.broadcast_to((x >= XH) & (x < XH + CX), shape)
        return jnp.minimum(low, jnp.where(own, k * inverse, 1.0))

    return plane


def lowest_of(low):
    low = jnp.min(low[YH : YH + CY], axis=0, keepdims=True)
    return jnp.broadcast_to(jnp.min(low, axis=1, keepdims=True), (1, 128))


def powers(ext, w, v):
    for x in range(1, EX - 1):
        v[0, x] = w[6, x] * ext[0, x]
    for n, width in enumerate((8, 11, 10, 9)):
        count = (EX - 4 - 2 * n) // width

        def several(m, _, n=n, width=width):
            for t in range(width):
                x = 2 + n + m * width + t
                mid = v[n, x]
                v[n + 1, x] = (
                    w[0, x] * v[n, x - 1]
                    + w[1, x] * v[n, x + 1]
                    + w[2, x] * pltpu.roll(mid, 1, 0)
                    + w[3, x] * pltpu.roll(mid, EY - 1, 0)
                    + w[4, x] * z_lower(mid)
                    + w[5, x] * z_upper(mid)
                )
            return 0

        lax.fori_loop(0, count, several, 0)


def incident(v, lows, inc):
    gx, gy = lax.axis_index("gx"), lax.axis_index("gy")
    shape = (EY, 128)
    lowest = jnp.min(lows[...], axis=0)
    delta = 1.0 - jnp.broadcast_to(lowest, shape)
    square = delta * delta
    scale = 1.0 / (16.0 - 20.0 * square + 5.0 * square * square)
    outer = 16.0 * scale
    inner = outer - 20.0 * square * scale
    row = lax.broadcasted_iota(jnp.int32, shape, 0)
    first_row = (row == YH - 1) & jnp.broadcast_to(gy == 0, shape)
    last_row = (row == YH + CY) & jnp.broadcast_to(gy == 7, shape)
    for x in range(CX + 2):
        at = x + XH - 1
        value = v[0, at] + inner * (v[1, at] + v[2, at]) + outer * (v[3, at] + v[4, at])
        value = jnp.where(first_row, pltpu.roll(value, EY - 1, 0), value)
        inc[x] = jnp.where(last_row, pltpu.roll(value, 1, 0), value)
    inc[0] = jnp.where(jnp.broadcast_to(gx == 0, shape), inc[1], inc[0])
    inc[CX + 1] = jnp.where(jnp.broadcast_to(gx == 15, shape), inc[CX], inc[CX + 1])


def make_select(keys_ref, table_ref):
    row = lax.broadcasted_iota(jnp.int32, (128, 256), 0)
    for h in range(2):
        key = keys_ref[h : h + 1, :]
        for v in range(BY):
            for l in range(6):
                taken = jnp.where(row == key - (l * 128 - 4 * v), 1.0, 0.0)
                table_ref[h, v, l * 128 : l * 128 + 128] = taken.astype(BF16)


def cut_windows(inc, table_ref, win):
    edge = lax.broadcasted_iota(jnp.int32, (32, 128), 0)
    both = []
    for h in range(2):
        pieces = [[] for _ in range(6)]
        for u in range(BX):
            stack = [inc[4 * u + 3 * h + i] for i in range(3)]
            stack = jnp.concatenate([*stack, jnp.zeros((8, 128), F32)], axis=0).T
            part = [stack[l * 32 : l * 32 + 32] for l in range(4)]
            pieces[0].append(jnp.where(edge == 0, part[0], pltpu.roll(part[3], 1, 0)))
            for l in range(4):
                pieces[l + 1].append(part[l])
            pieces[5].append(jnp.where(edge == 31, part[3], pltpu.roll(part[0], 31, 0)))
        rows = jnp.concatenate([jnp.concatenate(p, axis=0) for p in pieces], axis=1)
        both.append(jnp.concatenate(halves(rows), axis=0))
    for v in range(BY):
        value = dot(both[0], table_ref[0, v]) + dot(both[1], table_ref[1, v])
        top, rest = halves(value[:128] + value[128:])
        win[0, v * 128 : v * 128 + 128] = top
        win[1, v * 128 : v * 128 + 128] = rest


def pack_lines(block):
    top = block[:, :128].reshape(16, PAD, 128)[:, :CAP]
    rest = block[:, 128:].reshape(16, PAD, 128)
    last = rest[:, 8:].reshape(128, 128)
    moved = [pltpu.roll(last, 88 - 30 * p, 1).reshape(16, 8, 128) for p in range(3)]
    tail = [moved[n % 3][:, 1 + n // 3 : 2 + n // 3] for n in range(9)]
    lower = jnp.where(lanes((16, 9, 128)) < 88, rest[:, :9], jnp.concatenate(tail, axis=1))
    return top, lower


def unpack_lines(lines):
    lower = lines[:, CAP:]
    pieces = [
        jnp.concatenate([lower[:, 3 * j + p : 3 * j + p + 1] for j in range(3)], axis=1)
        for p in range(3)
    ]
    pieces = [pltpu.roll(x, (30 * p - 88) % 128, 2) for p, x in enumerate(pieces)]
    lane = lanes((16, 3, 128))
    last = jnp.where(lane < 30, pieces[0], jnp.where(lane < 60, pieces[1], pieces[2]))
    return padded_rows(lines[:, :CAP]), padded_rows(jnp.concatenate([lower, last], axis=1))


def couple_kernel(
    t_hbm, k_hbm, depth_hbm, boxes_hbm, places_hbm, average_hbm, keys_hbm,
    mine_ref, glow_ref, k_ref,
    t_ref, depth_ref, boxes_ref, places_ref, average_ref, keys_ref, select_ref,
    back_ref, target_ref, target_c, depths, held, source_ref, outgoing, arrived, grid_ref, hx, hy, hc, ext, w, v,
    low_ref, lows, inc, win, leaving,
    t_sem, k_sem, small_sem,
    out_send, out_recv, halo_send, halo_recv, low_send, low_recv, back_send, back_recv,
):
    me = lax.axis_index("gx") * 8 + lax.axis_index("gy")
    barrier = pltpu.get_barrier_semaphore()
    steps = SLOTS // ROWS

    def block_copies(step):
        rows = pl.ds(pl.multiple_of(step * ROWS, ROWS), ROWS)
        return (
            pltpu.make_async_copy(t_hbm.at[rows], t_ref.at[step % 3], t_sem.at[step]),
            pltpu.make_async_copy(k_hbm.at[rows], k_ref.at[rows], k_sem.at[step]),
        )

    small = [
        pltpu.make_async_copy(src, dst, small_sem.at[n])
        for n, (src, dst) in enumerate(
            (
                (depth_hbm, depth_ref),
                (boxes_hbm, boxes_ref),
                (places_hbm, places_ref),
                (average_hbm, average_ref),
                (keys_hbm, keys_ref),
            )
        )
    ]
    for copy in small[:3]:
        copy.start()
    for copy in (*block_copies(0), small[3], *block_copies(1)):
        copy.start()
    for who in peer_ids()[1:]:
        pl.semaphore_signal(barrier, inc=1, device_id=who, device_id_type=MESH)
    for copy in small[:3]:
        copy.wait()
    depth = depth_ref[...].astype(F32).reshape(1, SLOTS)
    for n in range(steps):
        depths[n : n + 1, :] = depth[:, n * ROWS : n * ROWS + ROWS]
    target_ref[...] = target_of(boxes_ref[...].reshape(1, SLOTS))
    small[3].wait()

    @pl.loop(0, steps)
    def _(step):
        @pl.when(step + 2 < steps)
        def _():
            for copy in block_copies(step + 2):
                copy.start()

        for copy in block_copies(step):
            copy.wait()
        restrict_block(step, t_ref, k_ref, depths, average_ref, glow_ref, held)

    high, low = halves(held[...])
    target = target_ref[...]
    base = place_index((256, 128), 0, me)
    pl.semaphore_wait(barrier, NDEV - 1)

    def to_owner(c):
        hot = one_hot(target, base, c)
        return dot(hot, high) + dot(hot, low)

    def put_out(c, block):
        outgoing[16 * c : 16 * c + 16] = block.reshape(16, PAD, 128)[:, :CAP]

    send_out(outgoing, to_owner, put_out, arrived, out_send, out_recv)
    small[4].start()
    source_ref[...] = source_of(places_ref[...].reshape(1, SLOTS))
    for n in range(steps):
        target_c[n * ROWS : n * ROWS + ROWS, :] = column(target[:, n * ROWS : n * ROWS + ROWS])
    source = source_ref[...]
    small[4].wait()
    make_select(keys_ref, select_ref)
    assemble(arrived, out_recv, source, base, grid_ref)
    ext[1, pl.ds(XH, CX), pl.ds(YH, CY)] = grid_ref[1]
    copies = [
        halo_copies(f, grid_ref, hx, hy, hc, halo_send, halo_recv) for f in range(2)
    ]
    for copy in copies[1]:
        copy.start()
    for copy in copies[1]:
        copy.wait_send()
    for copy in copies[0]:
        copy.start()
    plane = plane_coefficients(ext, w)
    for copy in copies[1][2:4]:
        copy.wait_recv()
    spread_y(1, ext, hy)
    low = lax.fori_loop(
        0,
        (CX - 2) // 2,
        lambda n, low: plane(XH + 2 + 2 * n, plane(XH + 1 + 2 * n, low)),
        jnp.ones((EY, 128), F32),
    )
    for copy in copies[1][:2]:
        copy.wait_recv()
    spread_near(ext, hx)
    low_ref[...] = lowest_of(plane(XH + CX - 1, plane(XH, low)))
    ext[0, pl.ds(XH, CX), pl.ds(YH, CY)] = grid_ref[0]
    ids = peer_ids()
    for q in sorted(range(1, NDEV), key=lambda q: -hops(q)):
        remote(low_ref, lows.at[q], low_send, low_recv, ids[q]).start()
    lows[0] = low_ref[...]
    for copy in copies[1][4:]:
        copy.wait_recv()
    spread_x(1, ext, hx, hc)

    def outer_pair(n, low):
        x = 1 + 2 * n + (CX - 2) * (n // 3)
        return plane(x + 1, plane(x, low))

    lax.fori_loop(0, XH, outer_pair, low)
    for copy in copies[0]:
        copy.wait()
    spread_y(0, ext, hy)
    spread_x(0, ext, hx, hc)
    powers(ext, w, v)
    others = pl.ds(1, NDEV - 1)
    pltpu.make_async_copy(lows.at[others], lows.at[others], low_recv).wait()
    incident(v, lows, inc)
    cut_windows(inc, select_ref, win)

    def to_slots(c):
        hot = one_hot(source, base, c)
        return dot(hot, win[0]) + dot(hot, win[1])

    def put_back(c, block):
        top, lower = pack_lines(block)
        leaving[16 * c : 16 * c + 16, :CAP] = top
        leaving[16 * c : 16 * c + 16, CAP:] = lower

    send_out(leaving, to_slots, put_back, back_ref, back_send, back_recv)
    across = place_index((1, 256), 1, me)
    for c in CHUNKS:
        wait_chunk(back_ref, back_recv, c)
        parts = [halves(part) for part in unpack_lines(back_ref[16 * c : 16 * c + 16])]
        rows = jnp.concatenate([part[k] for k in range(2) for part in parts], axis=1)
        index = jnp.bitwise_xor(across, c * PAD).astype(F32)
        for n in range(steps):
            at = slice(n * ROWS, n * ROWS + ROWS)
            hot = jnp.concatenate(
                [
                    jnp.where(
                        index[:, m * 128 : m * 128 + 128] == target_c[at, :], 1.0, 0.0
                    ).astype(BF16)
                    for m in range(2)
                ],
                axis=1,
            )
            found = dot(hot, rows).astype(BF16)
            mine_ref[at, :] = found if c == 0 else mine_ref[at, :] + found
    pltpu.make_async_copy(lows.at[others], lows.at[others], low_send).wait()
    pltpu.make_async_copy(outgoing.at[others], outgoing.at[others], out_send).wait()
    pltpu.make_async_copy(leaving.at[others], leaving.at[others], back_send).wait()


def prolong_kernel(mine_ref, k_ref, glow_ref, twice_ref, plane_ref, out_hbm, out_ref, sem):
    first = lanes((ROWS, 128)) < 64
    weights = line_weights()

    def copy_out(step):
        rows = pl.ds(pl.multiple_of(step * ROWS, ROWS), ROWS)
        return pltpu.make_async_copy(out_ref.at[rows], out_hbm.at[rows], sem.at[step])

    @pl.loop(0, SLOTS // ROWS)
    def _(step):
        at_row = pl.ds(pl.multiple_of(step * ROWS, ROWS), ROWS)
        both = dot(mine_ref[at_row, :], twice_ref[...])
        plane = plane_ref[...]
        for a in range(16):
            low = int(np.flatnonzero(weights[a])[0])
            value = float(weights[a, low]) * both[:, low * 128 : low * 128 + 128] + float(
                weights[a, low + 1]
            ) * both[:, low * 128 + 128 : low * 128 + 256]
            rest = value - value.astype(BF16).astype(F32)
            fine = dot(jnp.where(first, value, rest).astype(BF16), plane)
            at = slice(a * 256, a * 256 + 256)
            out_ref[at_row, at] = k_ref[at_row, at].astype(F32) * fine - glow_ref[at_row, at]
        copy_out(step).start()

    for step in range(SLOTS // ROWS):
        copy_out(step).wait()


VM = pl.BlockSpec(memory_space=pltpu.VMEM)
HB = pl.BlockSpec(memory_space=pltpu.HBM)
MIB = 1024 * 1024


def struct(*shape):
    return jax.ShapeDtypeStruct(shape, F32)


def on_device(thermal_state, opacity_field, glowing_depth, position_to_tile, tile_to_position):
    dma = pltpu.SemaphoreType.DMA
    steps = SLOTS // ROWS

    def vmem(*shape, dtype=F32):
        return pltpu.VMEM(shape, dtype)

    mine, glow, absorb = pl.pallas_call(
        couple_kernel,
        out_shape=[
            vmem(SLOTS, 512, dtype=BF16),
            vmem(SLOTS, 4096),
            vmem(SLOTS, 4096, dtype=BF16),
        ],
        in_specs=[HB] * 7,
        out_specs=[VM] * 3,
        scratch_shapes=[
            vmem(3, ROWS, 4096, dtype=BF16),
            vmem(SLOTS, dtype=jnp.int32),
            vmem(SLOTS, dtype=jnp.int32),
            vmem(SLOTS, dtype=jnp.int32),
            vmem(8, 256, 128, dtype=BF16),
            vmem(8, 256, dtype=jnp.int32),
            vmem(2, BY, 768, 256, dtype=BF16),
            vmem(NDEV, LINES, 128),
            vmem(1, SLOTS),
            vmem(SLOTS, 128),
            vmem(8, 128),
            vmem(SLOTS, 128),
            vmem(1, SLOTS),
            vmem(NDEV, CAP, 128),
            vmem(NDEV, CAP, 128),
            vmem(2, CX, CY, 128),
            vmem(2, 2, XH, CY, 128),
            vmem(2, 2, CX, YH, 128),
            vmem(2, 4, XH, YH, 128),
            vmem(2, EX, EY, 128),
            vmem(7, EX, EY, 128),
            vmem(5, EX, EY, 128),
            vmem(1, 128),
            vmem(NDEV, 1, 128),
            vmem(CX + 2, EY, 128),
            vmem(2, SLOTS, 256, dtype=BF16),
            vmem(NDEV, LINES, 128),
            dma((steps,)),
            dma((steps,)),
            dma((5,)),
            dma,
            dma((8,)),
            dma((2, 10)),
            dma((2, 10)),
            dma,
            dma,
            dma,
            dma((8,)),
        ],
        compiler_params=pltpu.CompilerParams(
            collective_id=0, has_side_effects=True, vmem_limit_bytes=30 * MIB
        ),
        name="couple",
    )(
        *(
            pltpu.with_memory_space_constraint(x, pltpu.HBM)
            for x in (
                thermal_state,
                opacity_field,
                glowing_depth,
                position_to_tile,
                tile_to_position,
                average_table(),
                select_keys(),
            )
        )
    )
    return pl.pallas_call(
        prolong_kernel,
        out_shape=struct(SLOTS, 4096),
        in_specs=[VM] * 5,
        out_specs=pl.BlockSpec(memory_space=pltpu.HBM),
        scratch_shapes=[vmem(SLOTS, 4096), dma((steps,))],
        compiler_params=pltpu.CompilerParams(vmem_limit_bytes=20 * MIB),
        name="prolong",
    )(
        *(pltpu.with_memory_space_constraint(x, pltpu.VMEM) for x in (mine, absorb, glow)),
        twice_table(),
        plane_table(),
    )


def solution(mesh):
    rows = P(("gx", "gy"), None)
    ints = P(("gx", "gy"))
    return jax.shard_map(
        on_device,
        mesh=mesh,
        in_specs=(rows, rows, ints, ints, ints),
        out_specs=rows,
        check_vma=False,
    )
```

```python
import jax
import jax.numpy as jnp
import numpy as np
from jax import lax
from jax.experimental import pallas as pl
from jax.experimental.pallas import tpu as pltpu
from jax.sharding import PartitionSpec as P

MESH = pl.DeviceIdType.MESH
F32 = jnp.float32
BF16 = jnp.bfloat16
BX, BY, BZ = 4, 6, 32
CX, CY = 16, 24
SLOTS = 768
NDEV = 128
CAP = 12
PAD = 16
LINES = 21
ROWS = 128
XH, YH = 6, 8
EX, EY = CX + 2 * XH, CY + 2 * YH


def average_table():
    table = np.zeros((4, 2, 2, 8, 16, 4, 2, 4, 4), np.float32)
    for i in range(4):
        for bh in range(2):
            for f in range(2):
                for b in range(8):
                    for c in range(16):
                        table[i, bh, f, b, c, c // 4, f, i, 2 * bh + b // 4] = 1.0 / 64.0
    return jnp.asarray(table.reshape(8, 256, 128), BF16)


def select_keys():
    keys = np.full((8, 256), -100000, np.int32)
    for n in range(216):
        i, j, l = n // 36, n % 36 // 6, n % 6
        keys[i // 3, n] = l * 128 + i % 3 * 40 + 7 + j
    return jnp.asarray(keys)


def twice_table():
    table = np.zeros((2, 256, 6, 2, 64), np.float32)
    for n in range(216):
        table[:, n, n // 36, :, n % 36] = 1.0
    return jnp.asarray(table.reshape(512, 768), BF16)


def line_weights():
    weights = np.zeros((16, 6))
    for a in range(16):
        position = (a + 0.5) / 4 + 0.5
        low = int(np.floor(position))
        weights[a, low] += 1.0 - (position - low)
        weights[a, low + 1] += position - low
    return weights


def plane_table():
    w = line_weights()
    plane = np.zeros((2, 64, 256))
    plane[:, :36] = np.kron(w, w).T
    return jnp.asarray(plane.reshape(128, 256), BF16)


def halves(x):
    high = x.astype(BF16)
    return high, (x - high.astype(F32)).astype(BF16)


def dot(a, b):
    return jnp.dot(a, b, preferred_element_type=F32)


def column(row):
    return jnp.broadcast_to(row, (128, 128)).T


def lanes(shape):
    return lax.broadcasted_iota(jnp.int32, shape, len(shape) - 1)


def flipped(x, k):
    return (x, x + 1 - 2 * (x % 2), (x + 2) % 4, 3 - x)[k]


def hops(q):
    near = (0, 1, 2, 1)
    return near[q // 32] + near[q // 8 % 4] + near[q // 2 % 4]


def peer_ids():
    gx, gy = lax.axis_index("gx"), lax.axis_index("gy")
    xs = [flipped(gx // 4, k) * 4 for k in range(4)]
    ys = [flipped(gx % 4, k) for k in range(4)]
    zs = [flipped(gy // 2, k) * 2 for k in range(4)]
    cs = [gy % 2, 1 - gy % 2]
    return [(xs[q // 32] + ys[q // 8 % 4], zs[q // 2 % 4] + cs[q % 2]) for q in range(NDEV)]


CHUNKS = range(8)
UPPER = [
    x * 64 + y * 16 + z * 4
    for x, y, z in (
        (1, 1, 1), (1, 1, 0), (1, 0, 1), (0, 1, 1), (1, 0, 0), (0, 1, 0), (0, 0, 1), (0, 0, 0)
    )
]
OWN = 112


def lower_bits(t):
    return t // 8 * 32 + t // 4 % 2 * 8 + t % 4


def peer_of(block):
    return UPPER[block // 16] + lower_bits(block % 16)


def chunk_blocks(c):
    return sorted(
        (n for n in range(16 * c, 16 * c + 16) if n != OWN), key=lambda n: -hops(peer_of(n))
    )


def place_index(shape, dim, me):
    row = lax.broadcasted_iota(jnp.int32, shape, dim)
    peer = jnp.bitwise_xor(lower_bits(row // PAD), jnp.broadcast_to(me, shape))
    return peer * PAD + row % PAD


def remote(src, dst, send_sem, recv_sem, who):
    return pltpu.make_async_remote_copy(
        src_ref=src,
        dst_ref=dst,
        send_sem=send_sem,
        recv_sem=recv_sem,
        device_id=who,
        device_id_type=MESH,
    )


def rank_row(owner, key):
    owner_c = [column(owner[:, i * 128 : i * 128 + 128]) for i in range(6)]
    key_c = [column(key[:, i * 128 : i * 128 + 128]) for i in range(6)]
    out = []
    for j in range(6):
        ro, rk = owner[:, j * 128 : j * 128 + 128], key[:, j * 128 : j * 128 + 128]
        total = jnp.zeros((128, 128), F32)
        for i in range(6):
            total += jnp.where((owner_c[i] == ro) & (key_c[i] < rk), 1.0, 0.0)
        out.append(jnp.sum(total, axis=0, keepdims=True))
    return jnp.concatenate(out, axis=1)


def target_of(box):
    box = box.astype(F32)
    owner = jnp.floor((box + 0.5) * (1.0 / SLOTS))
    return owner * PAD + rank_row(owner, lanes((1, SLOTS)).astype(F32))


def source_of(slot):
    slot = slot.astype(F32)
    home = jnp.floor((slot + 0.5) * (1.0 / SLOTS))
    rows = home * PAD + rank_row(home, slot)
    group = lanes((1, 128)) // 32
    out = []
    for v in range(BY):
        mixed = None
        for u in range(BX):
            at = u * BY + v
            part = rows[:, at // 4 * 128 : at // 4 * 128 + 128]
            part = pltpu.roll(part, (u - at) * 32 % 128, 1)
            mixed = part if mixed is None else jnp.where(group == u, part, mixed)
        out.append(mixed)
    return jnp.concatenate(out, axis=1)


def one_hot(row, base, c):
    index = jnp.bitwise_xor(base, UPPER[c] * PAD).astype(F32)
    return jnp.concatenate(
        [
            jnp.where(index == row[:, n * 128 : n * 128 + 128], 1.0, 0.0).astype(BF16)
            for n in range(SLOTS // 128)
        ],
        axis=1,
    )


def restrict_block(step, t_ref, k_ref, depths, table_ref, glow_ref, held):
    at_row = pl.ds(pl.multiple_of(step * ROWS, ROWS), ROWS)
    depth = column(depths[pl.ds(step, 1), :])
    layer = (lanes((ROWS, 128)) % 16).astype(F32)
    mask = jnp.where(layer < depth, 4.0, 0.0)
    total = jnp.zeros((ROWS, 128), F32)
    for i in range(4):
        for bh in range(2):
            glow = absorb = None
            for a in range(4):
                at = (4 * i + a) * 256 + bh * 128
                t = t_ref[step % 3, :, at : at + 128].astype(F32)
                k = k_ref[at_row, at : at + 128].astype(F32)
                square = t * t
                term = k * (square * square) * mask
                glow_ref[at_row, at : at + 128] = term
                glow = term if glow is None else glow + term
                absorb = k if absorb is None else absorb + k
            high, low = halves(jnp.concatenate([glow, absorb], axis=1))
            table = table_ref[2 * i + bh]
            total += dot(high, table) + dot(low, table)
    held[at_row, :] = total


def send_out(x_ref, make_block, put, o_ref, send_sem, recv_sems):
    ids = peer_ids()
    before = None
    for c in (*CHUNKS, None):
        if c is not None:
            put(c, make_block(c))
        if before is not None:
            for n in chunk_blocks(before):
                remote(
                    x_ref.at[n], o_ref.at[n], send_sem, recv_sems.at[before], ids[peer_of(n)]
                ).start()
        before = c
    o_ref[OWN] = x_ref[OWN]


def wait_chunk(o_ref, recv_sems, c):
    blocks = pl.ds(OWN + 1, 15) if c == OWN // 16 else pl.ds(16 * c, 16)
    pltpu.make_async_copy(o_ref.at[blocks], o_ref.at[blocks], recv_sems.at[c]).wait()


def padded_rows(value):
    n = value.shape[0]
    zeros = jnp.zeros((n, PAD - CAP, 128), F32)
    return jnp.concatenate([value, zeros], axis=1).reshape(n * PAD, 128)


def assemble(arrived, recv_sems, source, base, grid_ref):
    total = jnp.zeros((128, SLOTS), F32)
    for c in CHUNKS:
        wait_chunk(arrived, recv_sems, c)
        rows = padded_rows(arrived[16 * c : 16 * c + 16])
        high, low = halves(jnp.concatenate([rows[:128].T, rows[128:].T], axis=1))
        hot = one_hot(source, base, c)
        total += dot(high, hot) + dot(low, hot)
    group = lanes((32, 128)) // 32
    for v in range(BY):
        for u in range(BX):
            out = None
            for l in range(4):
                part = total[l * 32 : l * 32 + 32, v * 128 : v * 128 + 128]
                part = pltpu.roll(part, (l - u) * 32 % 128, 1)
                out = part if out is None else jnp.where(group == l, part, out)
            for f in range(2):
                for i in range(4):
                    at = (f * 4 + i) * 4
                    grid_ref[f, 4 * u + i, 4 * v : 4 * v + 4, :] = out[at : at + 4]


def halo_copies(f, grid_ref, hx_ref, hy_ref, hc_ref, send_sem, recv_sem):
    gx, gy = lax.axis_index("gx"), lax.axis_index("gy")
    up_x, down_x = (gx + 1) % 16, (gx + 15) % 16
    up_y, down_y = (gy + 1) % 8, (gy + 7) % 8
    last_y, first_y = pl.ds(CY - YH, YH), pl.ds(0, YH)
    deep = XH if f else XH - 1
    low, high = pl.ds(XH - deep, deep), pl.ds(0, deep)
    sent_low, sent_high = pl.ds(CX - deep, deep), pl.ds(0, deep)
    plan = [
        (grid_ref.at[f, :, last_y], hy_ref.at[f, 0], (gx, up_y)),
        (grid_ref.at[f, :, first_y], hy_ref.at[f, 1], (gx, down_y)),
        (grid_ref.at[f, sent_low, last_y], hc_ref.at[f, 0, low], (up_x, up_y)),
        (grid_ref.at[f, sent_low, first_y], hc_ref.at[f, 1, low], (up_x, down_y)),
        (grid_ref.at[f, sent_high, last_y], hc_ref.at[f, 2, high], (down_x, up_y)),
        (grid_ref.at[f, sent_high, first_y], hc_ref.at[f, 3, high], (down_x, down_y)),
    ]
    if f:
        near = [
            (grid_ref.at[f, pl.ds(CX - 1, 1)], hx_ref.at[f, 0, pl.ds(XH - 1, 1)], (up_x, gy)),
            (grid_ref.at[f, pl.ds(0, 1)], hx_ref.at[f, 1, pl.ds(0, 1)], (down_x, gy)),
        ]
        far = [
            (grid_ref.at[f, pl.ds(CX - XH, XH - 1)], hx_ref.at[f, 0, pl.ds(0, XH - 1)], (up_x, gy)),
            (grid_ref.at[f, pl.ds(1, XH - 1)], hx_ref.at[f, 1, pl.ds(1, XH - 1)], (down_x, gy)),
        ]
        plan = near + plan[:2] + far + plan[2:]
    else:
        plan = plan + [
            (grid_ref.at[f, sent_low], hx_ref.at[f, 0, low], (up_x, gy)),
            (grid_ref.at[f, sent_high], hx_ref.at[f, 1, high], (down_x, gy)),
        ]
    return [
        remote(src, dst, send_sem.at[f, n], recv_sem.at[f, n], who)
        for n, (src, dst, who) in enumerate(plan)
    ]


def spread_y(f, ext, hy_ref):
    for side, at in ((0, 0), (1, YH + CY)):
        ext[f, pl.ds(XH, CX), pl.ds(at, YH)] = hy_ref[f, side]


def spread_near(ext, hx_ref):
    own_y = pl.ds(YH, CY)
    ext[1, XH - 1, own_y] = hx_ref[1, 0, XH - 1]
    ext[1, XH + CX, own_y] = hx_ref[1, 1, 0]


def spread_x(f, ext, hx_ref, hc_ref):
    deep = XH if f else XH - 1
    for side, skip, at in ((0, XH - deep, XH - deep), (1, 0, XH + CX)):
        planes, from_planes = pl.ds(at, deep), pl.ds(skip, deep)
        ext[f, planes, pl.ds(YH, CY)] = hx_ref[f, side, from_planes]
        ext[f, planes, pl.ds(0, YH)] = hc_ref[f, 2 * side, from_planes]
        ext[f, planes, pl.ds(YH + CY, YH)] = hc_ref[f, 2 * side + 1, from_planes]


def z_lower(v):
    lane = lanes(v.shape)
    return jnp.where(lane < 32, pltpu.roll(v, 33, 1), pltpu.roll(v, 32, 1))


def z_upper(v):
    lane = lanes(v.shape)
    return jnp.where(lane >= 96, pltpu.roll(v, 95, 1), pltpu.roll(v, 96, 1))


def face(a, b):
    return (2.0 / 3.0) / (a + b)


def plane_coefficients(ext, w):
    gx, gy = lax.axis_index("gx"), lax.axis_index("gy")
    shape = (EY, 128)
    row = lax.broadcasted_iota(jnp.int32, shape, 0)
    lane = lanes(shape)
    y_at = gy * CY + row - YH
    has_ym, has_yp = y_at >= 1, y_at <= 8 * CY - 2
    has_zm, has_zp = lane != 0, lane != 127

    def plane(x, low):
        x_at = gx * CX + x - XH
        k = ext[1, x]
        has_xm = jnp.broadcast_to(x_at, shape) >= 1
        has_xp = jnp.broadcast_to(x_at, shape) <= 16 * CX - 2
        near = (
            (has_xm, ext[1, x - 1]),
            (has_xp, ext[1, x + 1]),
            (has_ym, pltpu.roll(k, 1, 0)),
            (has_yp, pltpu.roll(k, EY - 1, 0)),
            (has_zm, z_lower(k)),
            (has_zp, z_upper(k)),
        )
        faces = [face(k, jnp.where(has, other, k)) for has, other in near]
        diagonal = k
        for c in faces:
            diagonal = diagonal + c
        inverse = 1.0 / diagonal
        for n, c in enumerate(faces):
            w[n, x] = jnp.where(near[n][0], c * inverse, 0.0)
        w[6, x] = inverse
        own = jnp.broadcast_to((x >= XH) & (x < XH + CX), shape)
        return jnp.minimum(low, jnp.where(own, k * inverse, 1.0))

    return plane


def lowest_of(low):
    low = jnp.min(low[YH : YH + CY], axis=0, keepdims=True)
    return jnp.broadcast_to(jnp.min(low, axis=1, keepdims=True), (1, 128))


def powers(ext, w, v):
    for x in range(1, EX - 1):
        v[0, x] = w[6, x] * ext[0, x]
    for n, width in enumerate((8, 11, 10, 9)):
        count = (EX - 4 - 2 * n) // width

        def several(m, _, n=n, width=width):
            for t in range(width):
                x = 2 + n + m * width + t
                mid = v[n, x]
                v[n + 1, x] = (
                    w[0, x] * v[n, x - 1]
                    + w[1, x] * v[n, x + 1]
                    + w[2, x] * pltpu.roll(mid, 1, 0)
                    + w[3, x] * pltpu.roll(mid, EY - 1, 0)
                    + w[4, x] * z_lower(mid)
                    + w[5, x] * z_upper(mid)
                )
            return 0

        lax.fori_loop(0, count, several, 0)


def incident(v, lows, inc):
    gx, gy = lax.axis_index("gx"), lax.axis_index("gy")
    shape = (EY, 128)
    lowest = jnp.min(lows[...], axis=0)
    delta = 1.0 - jnp.broadcast_to(lowest, shape)
    square = delta * delta
    scale = 1.0 / (16.0 - 20.0 * square + 5.0 * square * square)
    outer = 16.0 * scale
    inner = outer - 20.0 * square * scale
    row = lax.broadcasted_iota(jnp.int32, shape, 0)
    first_row = (row == YH - 1) & jnp.broadcast_to(gy == 0, shape)
    last_row = (row == YH + CY) & jnp.broadcast_to(gy == 7, shape)
    for x in range(CX + 2):
        at = x + XH - 1
        value = v[0, at] + inner * (v[1, at] + v[2, at]) + outer * (v[3, at] + v[4, at])
        value = jnp.where(first_row, pltpu.roll(value, EY - 1, 0), value)
        inc[x] = jnp.where(last_row, pltpu.roll(value, 1, 0), value)
    inc[0] = jnp.where(jnp.broadcast_to(gx == 0, shape), inc[1], inc[0])
    inc[CX + 1] = jnp.where(jnp.broadcast_to(gx == 15, shape), inc[CX], inc[CX + 1])


def make_select(keys_ref, table_ref):
    row = lax.broadcasted_iota(jnp.int32, (128, 256), 0)
    for h in range(2):
        key = keys_ref[h : h + 1, :]
        for v in range(BY):
            for l in range(6):
                taken = jnp.where(row == key - (l * 128 - 4 * v), 1.0, 0.0)
                table_ref[h, v, l * 128 : l * 128 + 128] = taken.astype(BF16)


def cut_windows(inc, table_ref, win):
    edge = lax.broadcasted_iota(jnp.int32, (32, 128), 0)
    both = []
    for h in range(2):
        pieces = [[] for _ in range(6)]
        for u in range(BX):
            stack = [inc[4 * u + 3 * h + i] for i in range(3)]
            stack = jnp.concatenate([*stack, jnp.zeros((8, 128), F32)], axis=0).T
            part = [stack[l * 32 : l * 32 + 32] for l in range(4)]
            pieces[0].append(jnp.where(edge == 0, part[0], pltpu.roll(part[3], 1, 0)))
            for l in range(4):
                pieces[l + 1].append(part[l])
            pieces[5].append(jnp.where(edge == 31, part[3], pltpu.roll(part[0], 31, 0)))
        rows = jnp.concatenate([jnp.concatenate(p, axis=0) for p in pieces], axis=1)
        both.append(jnp.concatenate(halves(rows), axis=0))
    for v in range(BY):
        value = dot(both[0], table_ref[0, v]) + dot(both[1], table_ref[1, v])
        top, rest = halves(value[:128] + value[128:])
        win[0, v * 128 : v * 128 + 128] = top
        win[1, v * 128 : v * 128 + 128] = rest


def pack_lines(block):
    top = block[:, :128].reshape(16, PAD, 128)[:, :CAP]
    rest = block[:, 128:].reshape(16, PAD, 128)
    last = rest[:, 8:].reshape(128, 128)
    moved = [pltpu.roll(last, 88 - 30 * p, 1).reshape(16, 8, 128) for p in range(3)]
    tail = [moved[n % 3][:, 1 + n // 3 : 2 + n // 3] for n in range(9)]
    lower = jnp.where(lanes((16, 9, 128)) < 88, rest[:, :9], jnp.concatenate(tail, axis=1))
    return top, lower


def unpack_lines(lines):
    lower = lines[:, CAP:]
    pieces = [
        jnp.concatenate([lower[:, 3 * j + p : 3 * j + p + 1] for j in range(3)], axis=1)
        for p in range(3)
    ]
    pieces = [pltpu.roll(x, (30 * p - 88) % 128, 2) for p, x in enumerate(pieces)]
    lane = lanes((16, 3, 128))
    last = jnp.where(lane < 30, pieces[0], jnp.where(lane < 60, pieces[1], pieces[2]))
    return padded_rows(lines[:, :CAP]), padded_rows(jnp.concatenate([lower, last], axis=1))


def couple_kernel(
    t_hbm, k_hbm, depth_hbm, boxes_hbm, places_hbm, average_hbm, keys_hbm,
    mine_ref, glow_ref, k_ref,
    t_ref, depth_ref, boxes_ref, places_ref, average_ref, keys_ref, select_ref,
    back_ref, target_ref, target_c, depths, held, source_ref, outgoing, arrived, grid_ref, hx, hy, hc, ext, w, v,
    low_ref, lows, inc, win, leaving,
    t_sem, k_sem, small_sem,
    out_send, out_recv, halo_send, halo_recv, low_send, low_recv, back_send, back_recv,
):
    me = lax.axis_index("gx") * 8 + lax.axis_index("gy")
    barrier = pltpu.get_barrier_semaphore()
    steps = SLOTS // ROWS

    def block_copies(step):
        rows = pl.ds(pl.multiple_of(step * ROWS, ROWS), ROWS)
        return (
            pltpu.make_async_copy(t_hbm.at[rows], t_ref.at[step % 3], t_sem.at[step]),
            pltpu.make_async_copy(k_hbm.at[rows], k_ref.at[rows], k_sem.at[step]),
        )

    small = [
        pltpu.make_async_copy(src, dst, small_sem.at[n])
        for n, (src, dst) in enumerate(
            (
                (depth_hbm, depth_ref),
                (boxes_hbm, boxes_ref),
                (places_hbm, places_ref),
                (average_hbm, average_ref),
                (keys_hbm, keys_ref),
            )
        )
    ]
    for copy in small[:3]:
        copy.start()
    for copy in (*block_copies(0), small[3], *block_copies(1)):
        copy.start()
    for who in peer_ids()[1:]:
        pl.semaphore_signal(barrier, inc=1, device_id=who, device_id_type=MESH)
    for copy in small[:3]:
        copy.wait()
    depth = depth_ref[...].astype(F32).reshape(1, SLOTS)
    for n in range(steps):
        depths[n : n + 1, :] = depth[:, n * ROWS : n * ROWS + ROWS]
    target_ref[...] = target_of(boxes_ref[...].reshape(1, SLOTS))
    small[3].wait()

    @pl.loop(0, steps)
    def _(step):
        @pl.when(step + 2 < steps)
        def _():
            for copy in block_copies(step + 2):
                copy.start()

        for copy in block_copies(step):
            copy.wait()
        restrict_block(step, t_ref, k_ref, depths, average_ref, glow_ref, held)

    high, low = halves(held[...])
    target = target_ref[...]
    base = place_index((256, 128), 0, me)
    pl.semaphore_wait(barrier, NDEV - 1)

    def to_owner(c):
        hot = one_hot(target, base, c)
        return dot(hot, high) + dot(hot, low)

    def put_out(c, block):
        outgoing[16 * c : 16 * c + 16] = block.reshape(16, PAD, 128)[:, :CAP]

    send_out(outgoing, to_owner, put_out, arrived, out_send, out_recv)
    small[4].start()
    source_ref[...] = source_of(places_ref[...].reshape(1, SLOTS))
    for n in range(steps):
        target_c[n * ROWS : n * ROWS + ROWS, :] = column(target[:, n * ROWS : n * ROWS + ROWS])
    source = source_ref[...]
    small[4].wait()
    make_select(keys_ref, select_ref)
    assemble(arrived, out_recv, source, base, grid_ref)
    ext[1, pl.ds(XH, CX), pl.ds(YH, CY)] = grid_ref[1]
    copies = [
        halo_copies(f, grid_ref, hx, hy, hc, halo_send, halo_recv) for f in range(2)
    ]
    for copy in copies[1]:
        copy.start()
    for copy in copies[1]:
        copy.wait_send()
    for copy in copies[0]:
        copy.start()
    plane = plane_coefficients(ext, w)
    for copy in copies[1][2:4]:
        copy.wait_recv()
    spread_y(1, ext, hy)
    low = lax.fori_loop(
        0,
        (CX - 2) // 2,
        lambda n, low: plane(XH + 2 + 2 * n, plane(XH + 1 + 2 * n, low)),
        jnp.ones((EY, 128), F32),
    )
    for copy in copies[1][:2]:
        copy.wait_recv()
    spread_near(ext, hx)
    low_ref[...] = lowest_of(plane(XH + CX - 1, plane(XH, low)))
    ext[0, pl.ds(XH, CX), pl.ds(YH, CY)] = grid_ref[0]
    ids = peer_ids()
    for q in sorted(range(1, NDEV), key=lambda q: -hops(q)):
        remote(low_ref, lows.at[q], low_send, low_recv, ids[q]).start()
    lows[0] = low_ref[...]
    for copy in copies[1][4:]:
        copy.wait_recv()
    spread_x(1, ext, hx, hc)

    def outer_pair(n, low):
        x = 1 + 2 * n + (CX - 2) * (n // 3)
        return plane(x + 1, plane(x, low))

    lax.fori_loop(0, XH, outer_pair, low)
    for copy in copies[0]:
        copy.wait()
    spread_y(0, ext, hy)
    spread_x(0, ext, hx, hc)
    powers(ext, w, v)
    others = pl.ds(1, NDEV - 1)
    pltpu.make_async_copy(lows.at[others], lows.at[others], low_recv).wait()
    incident(v, lows, inc)
    cut_windows(inc, select_ref, win)

    def to_slots(c):
        hot = one_hot(source, base, c)
        return dot(hot, win[0]) + dot(hot, win[1])

    def put_back(c, block):
        top, lower = pack_lines(block)
        leaving[16 * c : 16 * c + 16, :CAP] = top
        leaving[16 * c : 16 * c + 16, CAP:] = lower

    send_out(leaving, to_slots, put_back, back_ref, back_send, back_recv)
    across = place_index((1, 256), 1, me)
    for c in CHUNKS:
        wait_chunk(back_ref, back_recv, c)
        parts = [halves(part) for part in unpack_lines(back_ref[16 * c : 16 * c + 16])]
        rows = jnp.concatenate([part[k] for k in range(2) for part in parts], axis=1)
        index = jnp.bitwise_xor(across, UPPER[c] * PAD).astype(F32)
        for n in range(steps):
            at = slice(n * ROWS, n * ROWS + ROWS)
            hot = jnp.concatenate(
                [
                    jnp.where(
                        index[:, m * 128 : m * 128 + 128] == target_c[at, :], 1.0, 0.0
                    ).astype(BF16)
                    for m in range(2)
                ],
                axis=1,
            )
            found = dot(hot, rows).astype(BF16)
            mine_ref[at, :] = found if c == 0 else mine_ref[at, :] + found
    pltpu.make_async_copy(lows.at[others], lows.at[others], low_send).wait()
    pltpu.make_async_copy(outgoing.at[others], outgoing.at[others], out_send).wait()
    pltpu.make_async_copy(leaving.at[others], leaving.at[others], back_send).wait()


def prolong_kernel(mine_ref, k_ref, glow_ref, twice_ref, plane_ref, out_hbm, out_ref, sem):
    first = lanes((ROWS, 128)) < 64
    weights = line_weights()

    def copy_out(step):
        rows = pl.ds(pl.multiple_of(step * ROWS, ROWS), ROWS)
        return pltpu.make_async_copy(out_ref.at[rows], out_hbm.at[rows], sem.at[step])

    @pl.loop(0, SLOTS // ROWS)
    def _(step):
        at_row = pl.ds(pl.multiple_of(step * ROWS, ROWS), ROWS)
        both = dot(mine_ref[at_row, :], twice_ref[...])
        plane = plane_ref[...]
        for a in range(16):
            low = int(np.flatnonzero(weights[a])[0])
            value = float(weights[a, low]) * both[:, low * 128 : low * 128 + 128] + float(
                weights[a, low + 1]
            ) * both[:, low * 128 + 128 : low * 128 + 256]
            rest = value - value.astype(BF16).astype(F32)
            fine = dot(jnp.where(first, value, rest).astype(BF16), plane)
            at = slice(a * 256, a * 256 + 256)
            out_ref[at_row, at] = k_ref[at_row, at].astype(F32) * fine - glow_ref[at_row, at]
        copy_out(step).start()

    for step in range(SLOTS // ROWS):
        copy_out(step).wait()


VM = pl.BlockSpec(memory_space=pltpu.VMEM)
HB = pl.BlockSpec(memory_space=pltpu.HBM)
MIB = 1024 * 1024


def struct(*shape):
    return jax.ShapeDtypeStruct(shape, F32)


def on_device(thermal_state, opacity_field, glowing_depth, position_to_tile, tile_to_position):
    dma = pltpu.SemaphoreType.DMA
    steps = SLOTS // ROWS

    def vmem(*shape, dtype=F32):
        return pltpu.VMEM(shape, dtype)

    mine, glow, absorb = pl.pallas_call(
        couple_kernel,
        out_shape=[
            vmem(SLOTS, 512, dtype=BF16),
            vmem(SLOTS, 4096),
            vmem(SLOTS, 4096, dtype=BF16),
        ],
        in_specs=[HB] * 7,
        out_specs=[VM] * 3,
        scratch_shapes=[
            vmem(3, ROWS, 4096, dtype=BF16),
            vmem(SLOTS, dtype=jnp.int32),
            vmem(SLOTS, dtype=jnp.int32),
            vmem(SLOTS, dtype=jnp.int32),
            vmem(8, 256, 128, dtype=BF16),
            vmem(8, 256, dtype=jnp.int32),
            vmem(2, BY, 768, 256, dtype=BF16),
            vmem(NDEV, LINES, 128),
            vmem(1, SLOTS),
            vmem(SLOTS, 128),
            vmem(8, 128),
            vmem(SLOTS, 128),
            vmem(1, SLOTS),
            vmem(NDEV, CAP, 128),
            vmem(NDEV, CAP, 128),
            vmem(2, CX, CY, 128),
            vmem(2, 2, XH, CY, 128),
            vmem(2, 2, CX, YH, 128),
            vmem(2, 4, XH, YH, 128),
            vmem(2, EX, EY, 128),
            vmem(7, EX, EY, 128),
            vmem(5, EX, EY, 128),
            vmem(1, 128),
            vmem(NDEV, 1, 128),
            vmem(CX + 2, EY, 128),
            vmem(2, SLOTS, 256, dtype=BF16),
            vmem(NDEV, LINES, 128),
            dma((steps,)),
            dma((steps,)),
            dma((5,)),
            dma,
            dma((8,)),
            dma((2, 10)),
            dma((2, 10)),
            dma,
            dma,
            dma,
            dma((8,)),
        ],
        compiler_params=pltpu.CompilerParams(
            collective_id=0, has_side_effects=True, vmem_limit_bytes=30 * MIB
        ),
        name="couple",
    )(
        *(
            pltpu.with_memory_space_constraint(x, pltpu.HBM)
            for x in (
                thermal_state,
                opacity_field,
                glowing_depth,
                position_to_tile,
                tile_to_position,
                average_table(),
                select_keys(),
            )
        )
    )
    return pl.pallas_call(
        prolong_kernel,
        out_shape=struct(SLOTS, 4096),
        in_specs=[VM] * 5,
        out_specs=pl.BlockSpec(memory_space=pltpu.HBM),
        scratch_shapes=[vmem(SLOTS, 4096), dma((steps,))],
        compiler_params=pltpu.CompilerParams(vmem_limit_bytes=20 * MIB),
        name="prolong",
    )(
        *(pltpu.with_memory_space_constraint(x, pltpu.VMEM) for x in (mine, absorb, glow)),
        twice_table(),
        plane_table(),
    )


def solution(mesh):
    rows = P(("gx", "gy"), None)
    ints = P(("gx", "gy"))
    return jax.shard_map(
        on_device,
        mesh=mesh,
        in_specs=(rows, rows, ints, ints, ints),
        out_specs=rows,
        check_vma=False,
    )
```

```python
import random

import jax
import jax.numpy as jnp
import numpy as np
from jax import lax
from jax.experimental import pallas as pl
from jax.experimental.pallas import tpu as pltpu
from jax.sharding import PartitionSpec as P

MESH = pl.DeviceIdType.MESH
F32 = jnp.float32
BF16 = jnp.bfloat16
BX, BY, BZ = 4, 6, 32
CX, CY = 16, 24
SLOTS = 768
NDEV = 128
CAP = 12
PAD = 16
LINES = 21
ROWS = 128
XH, YH = 6, 8
EX, EY = CX + 2 * XH, CY + 2 * YH


def average_table():
    table = np.zeros((4, 2, 2, 8, 16, 4, 2, 4, 4), np.float32)
    for i in range(4):
        for bh in range(2):
            for f in range(2):
                for b in range(8):
                    for c in range(16):
                        table[i, bh, f, b, c, c // 4, f, i, 2 * bh + b // 4] = 1.0 / 64.0
    return jnp.asarray(table.reshape(8, 256, 128), BF16)


def select_keys():
    keys = np.full((8, 256), -100000, np.int32)
    for n in range(216):
        i, j, l = n // 36, n % 36 // 6, n % 6
        keys[i // 3, n] = l * 128 + i % 3 * 40 + 7 + j
    return jnp.asarray(keys)


def twice_table():
    table = np.zeros((2, 256, 6, 2, 64), np.float32)
    for n in range(216):
        table[:, n, n // 36, :, n % 36] = 1.0
    return jnp.asarray(table.reshape(512, 768), BF16)


def line_weights():
    weights = np.zeros((16, 6))
    for a in range(16):
        position = (a + 0.5) / 4 + 0.5
        low = int(np.floor(position))
        weights[a, low] += 1.0 - (position - low)
        weights[a, low + 1] += position - low
    return weights


def plane_table():
    w = line_weights()
    plane = np.zeros((2, 64, 256))
    plane[:, :36] = np.kron(w, w).T
    return jnp.asarray(plane.reshape(128, 256), BF16)


def halves(x):
    high = x.astype(BF16)
    return high, (x - high.astype(F32)).astype(BF16)


def dot(a, b):
    return jnp.dot(a, b, preferred_element_type=F32)


def column(row):
    return jnp.broadcast_to(row, (128, 128)).T


def lanes(shape):
    return lax.broadcasted_iota(jnp.int32, shape, len(shape) - 1)


def flipped(x, k):
    return (x, x + 1 - 2 * (x % 2), (x + 2) % 4, 3 - x)[k]


def hops(q):
    near = (0, 1, 2, 1)
    return near[q // 32] + near[q // 8 % 4] + near[q // 2 % 4]


def peer_ids():
    gx, gy = lax.axis_index("gx"), lax.axis_index("gy")
    xs = [flipped(gx // 4, k) * 4 for k in range(4)]
    ys = [flipped(gx % 4, k) for k in range(4)]
    zs = [flipped(gy // 2, k) * 2 for k in range(4)]
    cs = [gy % 2, 1 - gy % 2]
    return [(xs[q // 32] + ys[q // 8 % 4], zs[q // 2 % 4] + cs[q % 2]) for q in range(NDEV)]


CHUNKS = range(8)


def peer_of(block):
    t = block % 16
    return t * 8 + (block // 16 ^ t % 8)


def chunk_blocks(c):
    blocks = [n for n in range(16 * c, 16 * c + 16) if n]
    random.Random(c).shuffle(blocks)
    return blocks


def place_index(shape, dim, me, start=0):
    row = lax.broadcasted_iota(jnp.int32, shape, dim) + start
    t = row // PAD % 16
    peer = jnp.bitwise_xor(t * 8 + jnp.bitwise_xor(t % 8, row // 256), jnp.broadcast_to(me, shape))
    return peer * PAD + row % PAD


def remote(src, dst, send_sem, recv_sem, who):
    return pltpu.make_async_remote_copy(
        src_ref=src,
        dst_ref=dst,
        send_sem=send_sem,
        recv_sem=recv_sem,
        device_id=who,
        device_id_type=MESH,
    )


def rank_row(owner, key):
    owner_c = [column(owner[:, i * 128 : i * 128 + 128]) for i in range(6)]
    key_c = [column(key[:, i * 128 : i * 128 + 128]) for i in range(6)]
    out = []
    for j in range(6):
        ro, rk = owner[:, j * 128 : j * 128 + 128], key[:, j * 128 : j * 128 + 128]
        total = jnp.zeros((128, 128), F32)
        for i in range(6):
            total += jnp.where((owner_c[i] == ro) & (key_c[i] < rk), 1.0, 0.0)
        out.append(jnp.sum(total, axis=0, keepdims=True))
    return jnp.concatenate(out, axis=1)


def target_of(box):
    box = box.astype(F32)
    owner = jnp.floor((box + 0.5) * (1.0 / SLOTS))
    return owner * PAD + rank_row(owner, lanes((1, SLOTS)).astype(F32))


def source_of(slot):
    slot = slot.astype(F32)
    home = jnp.floor((slot + 0.5) * (1.0 / SLOTS))
    rows = home * PAD + rank_row(home, slot)
    group = lanes((1, 128)) // 32
    out = []
    for v in range(BY):
        mixed = None
        for u in range(BX):
            at = u * BY + v
            part = rows[:, at // 4 * 128 : at // 4 * 128 + 128]
            part = pltpu.roll(part, (u - at) * 32 % 128, 1)
            mixed = part if mixed is None else jnp.where(group == u, part, mixed)
        out.append(mixed)
    return jnp.concatenate(out, axis=1)


def one_hot(row, base, c):
    index = jnp.bitwise_xor(base, c * PAD).astype(F32)
    return jnp.concatenate(
        [
            jnp.where(index == row[:, n * 128 : n * 128 + 128], 1.0, 0.0).astype(BF16)
            for n in range(SLOTS // 128)
        ],
        axis=1,
    )


def restrict_block(step, t_ref, k_ref, depths, table_ref, glow_ref, held):
    at_row = pl.ds(pl.multiple_of(step * ROWS, ROWS), ROWS)
    depth = column(depths[pl.ds(step, 1), :])
    layer = (lanes((ROWS, 128)) % 16).astype(F32)
    mask = jnp.where(layer < depth, 4.0, 0.0)
    total = jnp.zeros((ROWS, 128), F32)
    for i in range(4):
        for bh in range(2):
            glow = absorb = None
            for a in range(4):
                at = (4 * i + a) * 256 + bh * 128
                t = t_ref[step % 3, :, at : at + 128].astype(F32)
                k = k_ref[at_row, at : at + 128].astype(F32)
                square = t * t
                term = k * (square * square) * mask
                glow_ref[at_row, at : at + 128] = term
                glow = term if glow is None else glow + term
                absorb = k if absorb is None else absorb + k
            high, low = halves(jnp.concatenate([glow, absorb], axis=1))
            table = table_ref[2 * i + bh]
            total += dot(high, table) + dot(low, table)
    held[at_row, :] = total


def send_out(x_ref, make_block, put, o_ref, send_sem, recv_sems):
    ids = peer_ids()
    before = None
    for c in (*CHUNKS, None):
        if c is not None:
            put(c, make_block(c))
        if before is not None:
            for n in chunk_blocks(before):
                remote(
                    x_ref.at[n], o_ref.at[n], send_sem, recv_sems.at[before], ids[peer_of(n)]
                ).start()
        before = c
    o_ref[0] = x_ref[0]


def wait_chunk(o_ref, recv_sems, c):
    blocks = pl.ds(1, 15) if c == 0 else pl.ds(16 * c, 16)
    pltpu.make_async_copy(o_ref.at[blocks], o_ref.at[blocks], recv_sems.at[c]).wait()


def padded_rows(value):
    n = value.shape[0]
    zeros = jnp.zeros((n, PAD - CAP, 128), F32)
    return jnp.concatenate([value, zeros], axis=1).reshape(n * PAD, 128)


def assemble(arrived, recv_sems, source, base, grid_ref):
    total = jnp.zeros((128, SLOTS), F32)
    for c in CHUNKS:
        wait_chunk(arrived, recv_sems, c)
        rows = padded_rows(arrived[16 * c : 16 * c + 16])
        high, low = halves(jnp.concatenate([rows[:128].T, rows[128:].T], axis=1))
        hot = one_hot(source, base, c)
        total += dot(high, hot) + dot(low, hot)
    group = lanes((32, 128)) // 32
    for v in range(BY):
        for u in range(BX):
            out = None
            for l in range(4):
                part = total[l * 32 : l * 32 + 32, v * 128 : v * 128 + 128]
                part = pltpu.roll(part, (l - u) * 32 % 128, 1)
                out = part if out is None else jnp.where(group == l, part, out)
            for f in range(2):
                for i in range(4):
                    at = (f * 4 + i) * 4
                    grid_ref[f, 4 * u + i, 4 * v : 4 * v + 4, :] = out[at : at + 4]


def halo_copies(f, grid_ref, hx_ref, hy_ref, hc_ref, send_sem, recv_sem):
    gx, gy = lax.axis_index("gx"), lax.axis_index("gy")
    up_x, down_x = (gx + 1) % 16, (gx + 15) % 16
    up_y, down_y = (gy + 1) % 8, (gy + 7) % 8
    last_y, first_y = pl.ds(CY - YH, YH), pl.ds(0, YH)
    deep = XH if f else XH - 1
    low, high = pl.ds(XH - deep, deep), pl.ds(0, deep)
    sent_low, sent_high = pl.ds(CX - deep, deep), pl.ds(0, deep)
    plan = [
        (grid_ref.at[f, :, last_y], hy_ref.at[f, 0], (gx, up_y)),
        (grid_ref.at[f, :, first_y], hy_ref.at[f, 1], (gx, down_y)),
        (grid_ref.at[f, sent_low, last_y], hc_ref.at[f, 0, low], (up_x, up_y)),
        (grid_ref.at[f, sent_low, first_y], hc_ref.at[f, 1, low], (up_x, down_y)),
        (grid_ref.at[f, sent_high, last_y], hc_ref.at[f, 2, high], (down_x, up_y)),
        (grid_ref.at[f, sent_high, first_y], hc_ref.at[f, 3, high], (down_x, down_y)),
    ]
    if f:
        near = [
            (grid_ref.at[f, pl.ds(CX - 1, 1)], hx_ref.at[f, 0, pl.ds(XH - 1, 1)], (up_x, gy)),
            (grid_ref.at[f, pl.ds(0, 1)], hx_ref.at[f, 1, pl.ds(0, 1)], (down_x, gy)),
        ]
        far = [
            (grid_ref.at[f, pl.ds(CX - XH, XH - 1)], hx_ref.at[f, 0, pl.ds(0, XH - 1)], (up_x, gy)),
            (grid_ref.at[f, pl.ds(1, XH - 1)], hx_ref.at[f, 1, pl.ds(1, XH - 1)], (down_x, gy)),
        ]
        plan = near + plan[:2] + far + plan[2:]
    else:
        plan = plan + [
            (grid_ref.at[f, sent_low], hx_ref.at[f, 0, low], (up_x, gy)),
            (grid_ref.at[f, sent_high], hx_ref.at[f, 1, high], (down_x, gy)),
        ]
    return [
        remote(src, dst, send_sem.at[f, n], recv_sem.at[f, n], who)
        for n, (src, dst, who) in enumerate(plan)
    ]


def spread_y(f, ext, hy_ref):
    for side, at in ((0, 0), (1, YH + CY)):
        ext[f, pl.ds(XH, CX), pl.ds(at, YH)] = hy_ref[f, side]


def spread_near(ext, hx_ref):
    own_y = pl.ds(YH, CY)
    ext[1, XH - 1, own_y] = hx_ref[1, 0, XH - 1]
    ext[1, XH + CX, own_y] = hx_ref[1, 1, 0]


def spread_x(f, ext, hx_ref, hc_ref):
    deep = XH if f else XH - 1
    for side, skip, at in ((0, XH - deep, XH - deep), (1, 0, XH + CX)):
        planes, from_planes = pl.ds(at, deep), pl.ds(skip, deep)
        ext[f, planes, pl.ds(YH, CY)] = hx_ref[f, side, from_planes]
        ext[f, planes, pl.ds(0, YH)] = hc_ref[f, 2 * side, from_planes]
        ext[f, planes, pl.ds(YH + CY, YH)] = hc_ref[f, 2 * side + 1, from_planes]


def z_lower(v):
    lane = lanes(v.shape)
    return jnp.where(lane < 32, pltpu.roll(v, 33, 1), pltpu.roll(v, 32, 1))


def z_upper(v):
    lane = lanes(v.shape)
    return jnp.where(lane >= 96, pltpu.roll(v, 95, 1), pltpu.roll(v, 96, 1))


def face(a, b):
    return (2.0 / 3.0) / (a + b)


def plane_coefficients(ext, w):
    gx, gy = lax.axis_index("gx"), lax.axis_index("gy")
    shape = (EY, 128)
    row = lax.broadcasted_iota(jnp.int32, shape, 0)
    lane = lanes(shape)
    y_at = gy * CY + row - YH
    has_ym, has_yp = y_at >= 1, y_at <= 8 * CY - 2
    has_zm, has_zp = lane != 0, lane != 127

    def plane(x, low):
        x_at = gx * CX + x - XH
        k = ext[1, x]
        has_xm = jnp.broadcast_to(x_at, shape) >= 1
        has_xp = jnp.broadcast_to(x_at, shape) <= 16 * CX - 2
        near = (
            (has_xm, ext[1, x - 1]),
            (has_xp, ext[1, x + 1]),
            (has_ym, pltpu.roll(k, 1, 0)),
            (has_yp, pltpu.roll(k, EY - 1, 0)),
            (has_zm, z_lower(k)),
            (has_zp, z_upper(k)),
        )
        faces = [face(k, jnp.where(has, other, k)) for has, other in near]
        diagonal = k
        for c in faces:
            diagonal = diagonal + c
        inverse = 1.0 / diagonal
        for n, c in enumerate(faces):
            w[n, x] = jnp.where(near[n][0], c * inverse, 0.0)
        w[6, x] = inverse
        own = jnp.broadcast_to((x >= XH) & (x < XH + CX), shape)
        return jnp.minimum(low, jnp.where(own, k * inverse, 1.0))

    return plane


def lowest_of(low):
    low = jnp.min(low[YH : YH + CY], axis=0, keepdims=True)
    return jnp.broadcast_to(jnp.min(low, axis=1, keepdims=True), (1, 128))


def powers(ext, w, v):
    for x in range(1, EX - 1):
        v[0, x] = w[6, x] * ext[0, x]
    for n, width in enumerate((8, 11, 10, 9)):
        count = (EX - 4 - 2 * n) // width

        def several(m, _, n=n, width=width):
            for t in range(width):
                x = 2 + n + m * width + t
                mid = v[n, x]
                v[n + 1, x] = (
                    w[0, x] * v[n, x - 1]
                    + w[1, x] * v[n, x + 1]
                    + w[2, x] * pltpu.roll(mid, 1, 0)
                    + w[3, x] * pltpu.roll(mid, EY - 1, 0)
                    + w[4, x] * z_lower(mid)
                    + w[5, x] * z_upper(mid)
                )
            return 0

        lax.fori_loop(0, count, several, 0)


def incident(v, lows, inc):
    gx, gy = lax.axis_index("gx"), lax.axis_index("gy")
    shape = (EY, 128)
    lowest = jnp.min(lows[...], axis=0)
    delta = 1.0 - jnp.broadcast_to(lowest, shape)
    square = delta * delta
    scale = 1.0 / (16.0 - 20.0 * square + 5.0 * square * square)
    outer = 16.0 * scale
    inner = outer - 20.0 * square * scale
    row = lax.broadcasted_iota(jnp.int32, shape, 0)
    first_row = (row == YH - 1) & jnp.broadcast_to(gy == 0, shape)
    last_row = (row == YH + CY) & jnp.broadcast_to(gy == 7, shape)
    for x in range(CX + 2):
        at = x + XH - 1
        value = v[0, at] + inner * (v[1, at] + v[2, at]) + outer * (v[3, at] + v[4, at])
        value = jnp.where(first_row, pltpu.roll(value, EY - 1, 0), value)
        inc[x] = jnp.where(last_row, pltpu.roll(value, 1, 0), value)
    inc[0] = jnp.where(jnp.broadcast_to(gx == 0, shape), inc[1], inc[0])
    inc[CX + 1] = jnp.where(jnp.broadcast_to(gx == 15, shape), inc[CX], inc[CX + 1])


def make_select(keys_ref, table_ref):
    row = lax.broadcasted_iota(jnp.int32, (128, 256), 0)
    for h in range(2):
        key = keys_ref[h : h + 1, :]
        for v in range(BY):
            for l in range(6):
                taken = jnp.where(row == key - (l * 128 - 4 * v), 1.0, 0.0)
                table_ref[h, v, l * 128 : l * 128 + 128] = taken.astype(BF16)


def cut_windows(inc, table_ref, win):
    edge = lax.broadcasted_iota(jnp.int32, (32, 128), 0)
    both = []
    for h in range(2):
        pieces = [[] for _ in range(6)]
        for u in range(BX):
            stack = [inc[4 * u + 3 * h + i] for i in range(3)]
            stack = jnp.concatenate([*stack, jnp.zeros((8, 128), F32)], axis=0).T
            part = [stack[l * 32 : l * 32 + 32] for l in range(4)]
            pieces[0].append(jnp.where(edge == 0, part[0], pltpu.roll(part[3], 1, 0)))
            for l in range(4):
                pieces[l + 1].append(part[l])
            pieces[5].append(jnp.where(edge == 31, part[3], pltpu.roll(part[0], 31, 0)))
        rows = jnp.concatenate([jnp.concatenate(p, axis=0) for p in pieces], axis=1)
        both.append(jnp.concatenate(halves(rows), axis=0))
    for v in range(BY):
        value = dot(both[0], table_ref[0, v]) + dot(both[1], table_ref[1, v])
        top, rest = halves(value[:128] + value[128:])
        win[0, v * 128 : v * 128 + 128] = top
        win[1, v * 128 : v * 128 + 128] = rest


def pack_lines(block):
    top = block[:, :128].reshape(16, PAD, 128)[:, :CAP]
    rest = block[:, 128:].reshape(16, PAD, 128)
    last = rest[:, 8:].reshape(128, 128)
    moved = [pltpu.roll(last, 88 - 30 * p, 1).reshape(16, 8, 128) for p in range(3)]
    tail = [moved[n % 3][:, 1 + n // 3 : 2 + n // 3] for n in range(9)]
    lower = jnp.where(lanes((16, 9, 128)) < 88, rest[:, :9], jnp.concatenate(tail, axis=1))
    return top, lower


def unpack_lines(lines):
    lower = lines[:, CAP:]
    pieces = [
        jnp.concatenate([lower[:, 3 * j + p : 3 * j + p + 1] for j in range(3)], axis=1)
        for p in range(3)
    ]
    pieces = [pltpu.roll(x, (30 * p - 88) % 128, 2) for p, x in enumerate(pieces)]
    lane = lanes((16, 3, 128))
    last = jnp.where(lane < 30, pieces[0], jnp.where(lane < 60, pieces[1], pieces[2]))
    return padded_rows(lines[:, :CAP]), padded_rows(jnp.concatenate([lower, last], axis=1))


def couple_kernel(
    t_hbm, k_hbm, depth_hbm, boxes_hbm, places_hbm, average_hbm, keys_hbm,
    mine_ref, glow_ref, k_ref,
    t_ref, depth_ref, boxes_ref, places_ref, average_ref, keys_ref, select_ref,
    back_ref, target_ref, target_c, depths, held, source_ref, outgoing, arrived, grid_ref, hx, hy, hc, ext, w, v,
    low_ref, lows, inc, win, leaving,
    t_sem, k_sem, small_sem,
    out_send, out_recv, halo_send, halo_recv, low_send, low_recv, back_send, back_recv,
):
    me = lax.axis_index("gx") * 8 + lax.axis_index("gy")
    barrier = pltpu.get_barrier_semaphore()
    steps = SLOTS // ROWS

    def block_copies(step):
        rows = pl.ds(pl.multiple_of(step * ROWS, ROWS), ROWS)
        return (
            pltpu.make_async_copy(t_hbm.at[rows], t_ref.at[step % 3], t_sem.at[step]),
            pltpu.make_async_copy(k_hbm.at[rows], k_ref.at[rows], k_sem.at[step]),
        )

    small = [
        pltpu.make_async_copy(src, dst, small_sem.at[n])
        for n, (src, dst) in enumerate(
            (
                (depth_hbm, depth_ref),
                (boxes_hbm, boxes_ref),
                (places_hbm, places_ref),
                (average_hbm, average_ref),
                (keys_hbm, keys_ref),
            )
        )
    ]
    for copy in small[:3]:
        copy.start()
    for copy in (*block_copies(0), small[3], *block_copies(1)):
        copy.start()
    for who in peer_ids()[1:]:
        pl.semaphore_signal(barrier, inc=1, device_id=who, device_id_type=MESH)
    for copy in small[:3]:
        copy.wait()
    depth = depth_ref[...].astype(F32).reshape(1, SLOTS)
    for n in range(steps):
        depths[n : n + 1, :] = depth[:, n * ROWS : n * ROWS + ROWS]
    target_ref[...] = target_of(boxes_ref[...].reshape(1, SLOTS))
    small[3].wait()

    @pl.loop(0, steps)
    def _(step):
        @pl.when(step + 2 < steps)
        def _():
            for copy in block_copies(step + 2):
                copy.start()

        for copy in block_copies(step):
            copy.wait()
        restrict_block(step, t_ref, k_ref, depths, average_ref, glow_ref, held)

    high, low = halves(held[...])
    target = target_ref[...]
    base = place_index((256, 128), 0, me)
    pl.semaphore_wait(barrier, NDEV - 1)

    def to_owner(c):
        hot = one_hot(target, base, c)
        return dot(hot, high) + dot(hot, low)

    def put_out(c, block):
        outgoing[16 * c : 16 * c + 16] = block.reshape(16, PAD, 128)[:, :CAP]

    send_out(outgoing, to_owner, put_out, arrived, out_send, out_recv)
    small[4].start()
    source_ref[...] = source_of(places_ref[...].reshape(1, SLOTS))
    for n in range(steps):
        target_c[n * ROWS : n * ROWS + ROWS, :] = column(target[:, n * ROWS : n * ROWS + ROWS])
    source = source_ref[...]
    small[4].wait()
    make_select(keys_ref, select_ref)
    assemble(arrived, out_recv, source, base, grid_ref)
    ext[1, pl.ds(XH, CX), pl.ds(YH, CY)] = grid_ref[1]
    copies = [
        halo_copies(f, grid_ref, hx, hy, hc, halo_send, halo_recv) for f in range(2)
    ]
    for copy in copies[1]:
        copy.start()
    for copy in copies[1]:
        copy.wait_send()
    for copy in copies[0]:
        copy.start()
    plane = plane_coefficients(ext, w)
    for copy in copies[1][2:4]:
        copy.wait_recv()
    spread_y(1, ext, hy)
    low = lax.fori_loop(
        0,
        (CX - 2) // 2,
        lambda n, low: plane(XH + 2 + 2 * n, plane(XH + 1 + 2 * n, low)),
        jnp.ones((EY, 128), F32),
    )
    for copy in copies[1][:2]:
        copy.wait_recv()
    spread_near(ext, hx)
    low_ref[...] = lowest_of(plane(XH + CX - 1, plane(XH, low)))
    ext[0, pl.ds(XH, CX), pl.ds(YH, CY)] = grid_ref[0]
    ids = peer_ids()
    for q in sorted(range(1, NDEV), key=lambda q: -hops(q)):
        remote(low_ref, lows.at[q], low_send, low_recv, ids[q]).start()
    lows[0] = low_ref[...]
    for copy in copies[1][4:]:
        copy.wait_recv()
    spread_x(1, ext, hx, hc)

    def outer_pair(n, low):
        x = 1 + 2 * n + (CX - 2) * (n // 3)
        return plane(x + 1, plane(x, low))

    lax.fori_loop(0, XH, outer_pair, low)
    for copy in copies[0]:
        copy.wait()
    spread_y(0, ext, hy)
    spread_x(0, ext, hx, hc)
    powers(ext, w, v)
    others = pl.ds(1, NDEV - 1)
    pltpu.make_async_copy(lows.at[others], lows.at[others], low_recv).wait()
    incident(v, lows, inc)
    cut_windows(inc, select_ref, win)

    def to_slots(c):
        hot = one_hot(source, base, c)
        return dot(hot, win[0]) + dot(hot, win[1])

    def put_back(c, block):
        top, lower = pack_lines(block)
        leaving[16 * c : 16 * c + 16, :CAP] = top
        leaving[16 * c : 16 * c + 16, CAP:] = lower

    send_out(leaving, to_slots, put_back, back_ref, back_send, back_recv)
    across = place_index((1, 256), 1, me)
    for c in CHUNKS:
        wait_chunk(back_ref, back_recv, c)
        parts = [halves(part) for part in unpack_lines(back_ref[16 * c : 16 * c + 16])]
        rows = jnp.concatenate([part[k] for k in range(2) for part in parts], axis=1)
        index = jnp.bitwise_xor(across, c * PAD).astype(F32)
        for n in range(steps):
            at = slice(n * ROWS, n * ROWS + ROWS)
            hot = jnp.concatenate(
                [
                    jnp.where(
                        index[:, m * 128 : m * 128 + 128] == target_c[at, :], 1.0, 0.0
                    ).astype(BF16)
                    for m in range(2)
                ],
                axis=1,
            )
            found = dot(hot, rows).astype(BF16)
            mine_ref[at, :] = found if c == 0 else mine_ref[at, :] + found
    pltpu.make_async_copy(lows.at[others], lows.at[others], low_send).wait()
    pltpu.make_async_copy(outgoing.at[others], outgoing.at[others], out_send).wait()
    pltpu.make_async_copy(leaving.at[others], leaving.at[others], back_send).wait()


def prolong_kernel(mine_ref, k_ref, glow_ref, twice_ref, plane_ref, out_hbm, out_ref, sem):
    first = lanes((ROWS, 128)) < 64
    weights = line_weights()

    def copy_out(step):
        rows = pl.ds(pl.multiple_of(step * ROWS, ROWS), ROWS)
        return pltpu.make_async_copy(out_ref.at[rows], out_hbm.at[rows], sem.at[step])

    @pl.loop(0, SLOTS // ROWS)
    def _(step):
        at_row = pl.ds(pl.multiple_of(step * ROWS, ROWS), ROWS)
        both = dot(mine_ref[at_row, :], twice_ref[...])
        plane = plane_ref[...]
        for a in range(16):
            low = int(np.flatnonzero(weights[a])[0])
            value = float(weights[a, low]) * both[:, low * 128 : low * 128 + 128] + float(
                weights[a, low + 1]
            ) * both[:, low * 128 + 128 : low * 128 + 256]
            rest = value - value.astype(BF16).astype(F32)
            fine = dot(jnp.where(first, value, rest).astype(BF16), plane)
            at = slice(a * 256, a * 256 + 256)
            out_ref[at_row, at] = k_ref[at_row, at].astype(F32) * fine - glow_ref[at_row, at]
        copy_out(step).start()

    for step in range(SLOTS // ROWS):
        copy_out(step).wait()


VM = pl.BlockSpec(memory_space=pltpu.VMEM)
HB = pl.BlockSpec(memory_space=pltpu.HBM)
MIB = 1024 * 1024


def struct(*shape):
    return jax.ShapeDtypeStruct(shape, F32)


def on_device(thermal_state, opacity_field, glowing_depth, position_to_tile, tile_to_position):
    dma = pltpu.SemaphoreType.DMA
    steps = SLOTS // ROWS

    def vmem(*shape, dtype=F32):
        return pltpu.VMEM(shape, dtype)

    mine, glow, absorb = pl.pallas_call(
        couple_kernel,
        out_shape=[
            vmem(SLOTS, 512, dtype=BF16),
            vmem(SLOTS, 4096),
            vmem(SLOTS, 4096, dtype=BF16),
        ],
        in_specs=[HB] * 7,
        out_specs=[VM] * 3,
        scratch_shapes=[
            vmem(3, ROWS, 4096, dtype=BF16),
            vmem(SLOTS, dtype=jnp.int32),
            vmem(SLOTS, dtype=jnp.int32),
            vmem(SLOTS, dtype=jnp.int32),
            vmem(8, 256, 128, dtype=BF16),
            vmem(8, 256, dtype=jnp.int32),
            vmem(2, BY, 768, 256, dtype=BF16),
            vmem(NDEV, LINES, 128),
            vmem(1, SLOTS),
            vmem(SLOTS, 128),
            vmem(8, 128),
            vmem(SLOTS, 128),
            vmem(1, SLOTS),
            vmem(NDEV, CAP, 128),
            vmem(NDEV, CAP, 128),
            vmem(2, CX, CY, 128),
            vmem(2, 2, XH, CY, 128),
            vmem(2, 2, CX, YH, 128),
            vmem(2, 4, XH, YH, 128),
            vmem(2, EX, EY, 128),
            vmem(7, EX, EY, 128),
            vmem(5, EX, EY, 128),
            vmem(1, 128),
            vmem(NDEV, 1, 128),
            vmem(CX + 2, EY, 128),
            vmem(2, SLOTS, 256, dtype=BF16),
            vmem(NDEV, LINES, 128),
            dma((steps,)),
            dma((steps,)),
            dma((5,)),
            dma,
            dma((8,)),
            dma((2, 10)),
            dma((2, 10)),
            dma,
            dma,
            dma,
            dma((8,)),
        ],
        compiler_params=pltpu.CompilerParams(
            collective_id=0, has_side_effects=True, vmem_limit_bytes=30 * MIB
        ),
        name="couple",
    )(
        *(
            pltpu.with_memory_space_constraint(x, pltpu.HBM)
            for x in (
                thermal_state,
                opacity_field,
                glowing_depth,
                position_to_tile,
                tile_to_position,
                average_table(),
                select_keys(),
            )
        )
    )
    return pl.pallas_call(
        prolong_kernel,
        out_shape=struct(SLOTS, 4096),
        in_specs=[VM] * 5,
        out_specs=pl.BlockSpec(memory_space=pltpu.HBM),
        scratch_shapes=[vmem(SLOTS, 4096), dma((steps,))],
        compiler_params=pltpu.CompilerParams(vmem_limit_bytes=20 * MIB),
        name="prolong",
    )(
        *(pltpu.with_memory_space_constraint(x, pltpu.VMEM) for x in (mine, absorb, glow)),
        twice_table(),
        plane_table(),
    )


def solution(mesh):
    rows = P(("gx", "gy"), None)
    ints = P(("gx", "gy"))
    return jax.shard_map(
        on_device,
        mesh=mesh,
        in_specs=(rows, rows, ints, ints, ints),
        out_specs=rows,
        check_vma=False,
    )
```
